128 devices in a mesh: ctx: 32 (over z, x, core), exp: 4 (over y).
Axes of the slice: x: 4, y: 4, z: 4, core: 2. Of those that a mesh axis runs over, the one named last changes fastest.
Arguments:
- queries: bfloat16 [4096, 4096], P('ctx', 'exp'), may hold values from -5 to 5
- keys: bfloat16 [4096, 1024], P('ctx', 'exp'), may hold values from -5 to 5
- values: bfloat16 [4096, 1024], P('ctx', 'exp'), may hold values from -6 to 6
- resid_in: bfloat16 [4096, 4096], P(('ctx', 'exp')), may hold values from -6 to 6
- span_order: int32 [64], replicated, may hold values from 0 to 63, each once
- out_weight: bfloat16 [4096, 4096], P('exp'), may hold values from -0.09375 to 0.09375
- norm_gain: float32 [4096], replicated, may hold values from 0.25 to 1.75
- router: float32 [4096, 4], replicated, may hold values from -0.09375 to 0.09375
- expert_ids: int32 [4096, 2], P(('ctx', 'exp')), may hold values from 0 to 3, all different within a row; in each aligned block of 32 rows (0 to 31, 32 to 63, ...) at most 16 rows name the same one
- w_gate: bfloat16 [4, 4096, 14336], P('exp', None, 'ctx'), may hold values from -0.09375 to 0.09375
- w_up: bfloat16 [4, 4096, 14336], P('exp', None, 'ctx'), may hold values from -0.09375 to 0.09375
- w_down: bfloat16 [4, 14336, 4096], P('exp', 'ctx'), may hold values from -0.046875 to 0.046875
Outputs:
- mixed: bfloat16 [4096, 4096], P(('ctx', 'exp'))
The draws below stay inside these ranges and needn't reach their ends.
Inputs may be any that keep to these rules, and one draw needn't show every extreme that they name: `expert_ids`: A token's 2 ids differ. In every aligned block of 32 tokens, each of the 4 experts is named by exactly 16 tokens. `span_order`: each span number appears once.
All inputs are finite; a program needn't handle non-finite values.
Results may differ from the reference program's by a relative error of at most 0.012.
Values may be sent and summed in bfloat16 or wider, within the bound.
No kernel may reach another device: no remote copies, remote signals or barrier semaphores. Data moves between devices by JAX's collectives and lax.ppermute only.
A program may use at most 128 MiB of HBM per device.

```python
import math
import jax
import jax.numpy as jnp
import numpy as np
from jax import lax

D = 4096
QUERY_HEADS = 32
KEY_VALUE_HEADS = 8
HEAD_SIZE = 128
FF = 14336
TOP = 2
SPAN = 64
EXPERTS = 4
SEQUENCE_TOKENS = 4096
SPANS = 64
SUB = 32
SLOT = 16
N_CTX = 32


def base_domain(key, salt, columns):
    return jnp.clip(jax.random.normal(jax.random.fold_in(key, salt), (SEQUENCE_TOKENS, columns), jnp.float32), -5.0, 5.0)


def with_labels(key, field):
    return field


def draw_queries(key, part):
    return with_labels(key, base_domain(key, 11, QUERY_HEADS * HEAD_SIZE)).astype(jnp.bfloat16)


def draw_keys(key, part):
    return with_labels(key, base_domain(key, 23, KEY_VALUE_HEADS * HEAD_SIZE)).astype(jnp.bfloat16)


def steps_of(stream_key, extent, cuts, low, largest):
    def one(axis_at, parts):
        steps = jax.random.uniform(jax.random.fold_in(jax.random.fold_in(stream_key, 6), axis_at), (parts,), jnp.float32, low / len(cuts), largest / len(cuts))
        return jnp.repeat(jnp.exp(steps), extent[axis_at] // parts).reshape((-1,) + (1,) * (len(extent) - axis_at - 1))

    factor_of = one(*cuts[0])
    for cut in cuts[1:]:
        factor_of = factor_of * one(*cut)
    return factor_of


def assign_block(own_key, own, number, rows, number_of, top, limit, slope):
    ranking = jax.random.permutation(own_key, number_of)
    heavy_load, common = load_shares(number_of, rows * top, limit, slope, True), load_shares(number_of, rows * top, limit, slope, False)
    places = jnp.arange(number_of)

    def named(tallies, turn):
        used = int((tallies > 0).sum())
        fixed = max(1, used // 4)
        shifted = fixed + (places - fixed + turn * (used - fixed)) % max(1, number_of - fixed)
        return jnp.zeros((number_of,), jnp.int32).at[ranking[jnp.where(places < fixed, places, shifted)]].set(jnp.asarray(tallies, jnp.int32))

    tallies = jnp.where(number % 4 == 0, named(heavy_load, number // 4), named(common, number - number // 4 - 1))
    mixed = jax.random.permutation(jax.random.fold_in(own, 3), number_of)
    giver, sink = mixed[0:number_of // 2 * 2:2], mixed[1:number_of // 2 * 2:2]
    room = jnp.minimum(tallies[giver] - 1, limit - tallies[sink]) // 2
    room = jnp.where((giver == ranking[0]) | (sink == ranking[0]) | (tallies[sink] == 0), 0, jnp.maximum(room, 0))
    shifted = jax.random.randint(jax.random.fold_in(own, 4), (number_of // 2,), 0, 1 << 20) % (room + 1)
    tallies = tallies.at[giver].add(-shifted).at[sink].add(shifted)
    items = jnp.searchsorted(jnp.cumsum(tallies), jnp.arange(rows * top), side="right").astype(jnp.int32)
    listing = items.reshape(top, rows).T
    listing = listing[jax.random.permutation(jax.random.fold_in(own, 1), rows)]
    turn = jax.random.randint(jax.random.fold_in(own, 2), (rows, 1), 0, top)
    return jnp.take_along_axis(listing, (jnp.arange(top)[None, :] + turn) % top, axis=1)


def load_shares(number_of, total, reach, slope, full):
    loads = [(1 << 20) // math.isqrt(rank ** slope) + 1 for rank in range(1, number_of + 1)]
    largest = reach if full else min(reach, max(-(-total // number_of), total * loads[0] // sum(loads)))
    least = 1 if total - largest >= number_of - 1 else 0
    counts, rest = [largest] + [least] * (number_of - 1), total - largest - least * (number_of - 1)
    while rest > 0:
        movable = [i for i in range(1, number_of) if counts[i] < largest] or [i for i in range(1, number_of) if counts[i] < reach]
        whole, left = sum([loads[i] for i in movable]), rest
        for i in movable:
            more = min(reach - counts[i], max(1, left * loads[i] // whole), rest)
            counts[i] = counts[i] + more
            rest = rest - more
    return np.array(counts)


def normal_values(rng, dims, deviation, most, cuts=(), kind=jnp.bfloat16):
    level = steps_of(rng, dims, cuts, -0.22, 0.18) if cuts else 1.0
    entries = jax.random.normal(rng, dims, jnp.float32) * deviation * level
    return jnp.minimum(jnp.maximum(entries, -most), most).astype(kind)


def setup_inputs(seed: int = 0) -> dict:
    arg_keys = jax.random.split(jax.random.key(seed), 13)
    queries = draw_queries(jax.random.fold_in(arg_keys[12], 71), 0)
    keys = draw_keys(jax.random.fold_in(arg_keys[12], 71), 0)
    values = normal_values(arg_keys[2], (SEQUENCE_TOKENS, KEY_VALUE_HEADS * HEAD_SIZE), 1.0, 6.0, ((0, 32), (1, 4)))
    resid_in = normal_values(arg_keys[3], (SEQUENCE_TOKENS, D), 1.0, 6.0, ((0, 128),))
    span_order = jax.random.permutation(arg_keys[4], SPANS).astype(jnp.int32)
    out_weight = normal_values(arg_keys[5], (QUERY_HEADS * HEAD_SIZE, D), (QUERY_HEADS * HEAD_SIZE) ** -0.5, 0.09375, ((0, 4),))
    norm_gain = jnp.clip(1.0 + 0.15 * jax.random.normal(arg_keys[6], (D,), jnp.float32), 0.25, 1.75)
    router = normal_values(arg_keys[7], (D, EXPERTS), D ** -0.5, 0.09375, (), jnp.float32)
    expert_ids_keys = jax.random.split(jax.random.fold_in(arg_keys[8], 1), SEQUENCE_TOKENS // SUB)
    expert_ids_turns = jax.random.permutation(jax.random.fold_in(arg_keys[8], 3), SEQUENCE_TOKENS // SUB)
    expert_ids = jax.vmap(lambda own, number: assign_block(jax.random.fold_in(arg_keys[8], 2), own, number, SUB, EXPERTS, TOP, SLOT, 0))(expert_ids_keys, expert_ids_turns).reshape((SEQUENCE_TOKENS, TOP))
    w_gate = normal_values(arg_keys[9], (EXPERTS, D, FF), D ** -0.5, 0.09375, ((0, 4), (2, 32)))
    w_up = normal_values(arg_keys[10], (EXPERTS, D, FF), D ** -0.5, 0.09375, ((0, 4), (2, 32)))
    w_down = normal_values(arg_keys[11], (EXPERTS, FF, D), FF ** -0.5, 0.046875, ((0, 4), (1, 32)))
    return {"queries": queries, "keys": keys, "values": values, "resid_in": resid_in, "span_order": span_order, "out_weight": out_weight, "norm_gain": norm_gain, "router": router, "expert_ids": expert_ids, "w_gate": w_gate, "w_up": w_up, "w_down": w_down}


def expert_rows(inputs, gate_mat, up_mat, down_mat):
    shard_width = FF // N_CTX

    def add_shard(summed, shard_no):
        offset = (shard_no * shard_width).astype(jnp.int32)
        gate_part = jnp.dot(inputs, lax.dynamic_slice_in_dim(gate_mat, offset, shard_width, 1), preferred_element_type=jnp.float32)
        up_part = jnp.dot(inputs, lax.dynamic_slice_in_dim(up_mat, offset, shard_width, 1), preferred_element_type=jnp.float32)
        hidden = (jax.nn.silu(gate_part) * up_part).astype(jnp.bfloat16)
        partial_out = jnp.dot(hidden, lax.dynamic_slice_in_dim(down_mat, offset, shard_width, 0), preferred_element_type=jnp.float32)
        rounded = lax.optimization_barrier(partial_out.astype(jnp.bfloat16))
        return (summed + rounded.astype(jnp.float32), None)
    start_sum = jnp.zeros((inputs.shape[0], D), jnp.float32)
    summed, _ = lax.scan(add_shard, start_sum, jnp.arange(N_CTX, dtype=jnp.int32))
    return summed.astype(jnp.bfloat16)

def reference(queries, keys, values, resid_in, span_order, out_weight, norm_gain, router, expert_ids, w_gate, w_up, w_down):
    stored = jnp.arange(SEQUENCE_TOKENS, dtype=jnp.int32)
    position = span_order[stored // SPAN] * SPAN + stored % SPAN
    allowed = position[None, :] <= position[:, None]
    head_cluster = QUERY_HEADS // KEY_VALUE_HEADS
    query_head_rows = jnp.transpose(queries.astype(jnp.float32).reshape(SEQUENCE_TOKENS, KEY_VALUE_HEADS, head_cluster, HEAD_SIZE), (1, 2, 0, 3))
    key_head_rows = jnp.transpose(keys.astype(jnp.float32).reshape(SEQUENCE_TOKENS, KEY_VALUE_HEADS, HEAD_SIZE), (1, 0, 2))
    value_head_rows = jnp.transpose(values.astype(jnp.float32).reshape(SEQUENCE_TOKENS, KEY_VALUE_HEADS, HEAD_SIZE), (1, 0, 2))

    def one_head(operands):
        query_one, key_one, value_one = operands
        scores = jnp.einsum('gqd,kd->gqk', query_one, key_one) / math.sqrt(HEAD_SIZE)
        scores = jnp.where(allowed[None], scores, -1e+30)
        row_max = lax.optimization_barrier(jnp.max(scores, axis=-1, keepdims=True))
        weights = jnp.where(allowed[None], jnp.exp(scores - row_max), 0.0)
        denominator = lax.optimization_barrier(jnp.sum(weights, axis=-1))
        rounded = lax.optimization_barrier(weights.astype(jnp.bfloat16)).astype(jnp.float32)
        numerator = jnp.einsum('gqk,kd->gqd', rounded, value_one)
        return numerator / denominator[..., None]
    heads_out = lax.map(one_head, (query_head_rows, key_head_rows, value_head_rows))
    attended = jnp.transpose(heads_out, (2, 0, 1, 3)).reshape(SEQUENCE_TOKENS, QUERY_HEADS * HEAD_SIZE).astype(jnp.bfloat16)
    projected = jnp.dot(attended, out_weight, preferred_element_type=jnp.float32)
    stream = (resid_in.astype(jnp.float32) + projected).astype(jnp.bfloat16)
    stream_wide = stream.astype(jnp.float32)
    mean_square = lax.optimization_barrier(jnp.mean(stream_wide * stream_wide, axis=-1, keepdims=True))
    normed = (stream_wide * lax.rsqrt(mean_square + 1e-05) * norm_gain).astype(jnp.bfloat16)
    logits = jnp.dot(normed.astype(jnp.float32), router, precision=lax.Precision.HIGHEST)
    chosen = jnp.take_along_axis(logits, expert_ids, axis=1)
    mixing = jax.nn.softmax(chosen, axis=-1)
    expert_total = jnp.zeros((SEQUENCE_TOKENS, D), jnp.float32)
    row_count = SEQUENCE_TOKENS * TOP // EXPERTS
    for expert in range(EXPERTS):
        matches = expert_ids == expert
        routed = jnp.any(matches, axis=1)
        token_weight = lax.optimization_barrier(jnp.sum(jnp.where(matches, mixing, 0.0), axis=1))
        indices = jnp.nonzero(routed, size=row_count)[0].astype(jnp.int32)
        outputs = expert_rows(normed[indices], w_gate[expert], w_up[expert], w_down[expert])
        expert_total = expert_total.at[indices].add(token_weight[indices][:, None] * outputs.astype(jnp.float32))
    return (stream_wide + expert_total).astype(jnp.bfloat16)
```

```python
import math

import jax
import jax.numpy as jnp
from jax import lax
from jax.sharding import PartitionSpec as P

HEAD_SIZE = 128
SPAN = 64
RING = 4

f32 = jnp.float32
bf16 = jnp.bfloat16


def ctx_index_of(z, x, core):
    return (z % RING) * 8 + (x % RING) * 2 + core


def ring_pairs(phase, step):
    pairs = []
    for z in range(RING):
        for x in range(RING):
            for core in range(2):
                along_x = (core == 0) == (phase == 1)
                target = ctx_index_of(z, x + step, core) if along_x else ctx_index_of(z + step, x, core)
                pairs.append((ctx_index_of(z, x, core), target))
    return pairs


RINGS = {(phase, step): ring_pairs(phase, step) for phase in (1, 2) for step in (1, -1, 2)}
SWAP = [(i, i ^ 1) for i in range(32)]


def shift(a, phase, step):
    return lax.ppermute(a, "ctx", RINGS[phase, step])


def swap(a):
    return lax.ppermute(a, "ctx", SWAP)


def shift_exp(a, step):
    return lax.ppermute(a, "exp", [(i, (i + step) % 4) for i in range(4)])


def join(*parts):
    return jnp.concatenate(parts, axis=0)


def total(*terms):
    return sum(t.astype(f32) for t in terms).astype(bf16)


def gather_direct(a, phase):
    return join(a, shift(a, phase, 1), shift(a, phase, -1), shift(a, phase, 2))


def gather_ring(a, phase):
    half = a.shape[0] // 2
    r = shift(a, phase, 1)
    l = shift(a, phase, -1)
    d0 = shift(r[:half], phase, 1)
    d1 = shift(l[half:], phase, -1)
    return join(a, r, l, d0, d1)


def gather_ring_split(a, phase):
    half = a.shape[0] // 2
    r0 = shift(a[:half], phase, 1)
    l1 = shift(a[half:], phase, -1)
    r1 = shift(a[half:], phase, 1)
    l0 = shift(a[:half], phase, -1)
    d0 = shift(r0, phase, 1)
    d1 = shift(l1, phase, -1)
    return join(r0, r1, l0, l1), join(d0, d1)


def sum_ring(own, minus, plus, far, phase):
    half = own.shape[0] // 2
    qm = shift(far[:half], phase, -1)
    qp = shift(far[half:], phase, 1)
    um = shift(join(total(minus[:half], qm), minus[half:]), phase, -1)
    up = shift(join(plus[:half], total(plus[half:], qp)), phase, 1)
    return own.astype(f32) + um.astype(f32) + up.astype(f32)


def sum_ring_split(own, minus, plus, far, phase):
    half = own.shape[0] // 2
    u1 = shift(minus[half:], phase, -1)
    v1 = shift(plus[:half], phase, 1)
    qm = shift(far[:half], phase, -1)
    qp = shift(far[half:], phase, 1)
    u2 = shift(total(minus[:half], qm), phase, -1)
    v2 = shift(total(plus[half:], qp), phase, 1)
    return join(total(own[:half], u2, v1), total(own[half:], u1, v2))


def quarters(a):
    n = a.shape[0] // 4
    return a[:n], a[n : 2 * n], a[2 * n : 3 * n], a[3 * n :]


def positions_of(span_ids, span_order):
    matches = span_ids[:, None] == jnp.arange(span_order.shape[0], dtype=jnp.int32)[None, :]
    starts = jnp.sum(jnp.where(matches, span_order[None, :], 0), axis=1) * SPAN
    return (starts[:, None] + jnp.arange(SPAN, dtype=jnp.int32)[None, :]).reshape(-1)


def on_device(
    queries,
    keys,
    values,
    resid_in,
    span_order,
    out_weight,
    norm_gain,
    router,
    expert_ids,
    w_gate,
    w_up,
    w_down,
):
    tok_rows = queries.shape[0]
    kv_heads = keys.shape[1] // HEAD_SIZE
    head_cluster = queries.shape[1] // HEAD_SIZE // kv_heads
    kv_width = keys.shape[1]
    me = lax.axis_index("ctx")
    mine = lax.axis_index("exp")
    my_z, my_x, my_core = me // 8, (me // 2) % RING, me % 2

    kv = jnp.concatenate((keys, values), axis=1)
    near = gather_direct(kv, 1)
    side, far = gather_ring_split(near, 2)
    both = join(near, swap(near), side, swap(side), far, swap(far))

    first = jnp.array([0, -1, 1, 2], jnp.int32)

    def sources(second, core):
        a, b = jnp.tile(first, second.shape[0]), jnp.repeat(second, 4)
        z = jnp.where(core == 0, my_z + b, my_z + a) % RING
        x = jnp.where(core == 0, my_x + a, my_x + b) % RING
        return z * 8 + x * 2 + core

    blocks = []
    for second in ([0], [-1, 1], [2]):
        second = jnp.array(second, jnp.int32)
        blocks += [sources(second, my_core), sources(second, 1 - my_core)]
    blocks = jnp.concatenate(blocks)
    key_spans = (blocks[:, None] * 2 + jnp.arange(2, dtype=jnp.int32)[None, :]).reshape(-1)
    key_pos = positions_of(key_spans, span_order)
    query_pos = positions_of(me * 2 + jnp.arange(2, dtype=jnp.int32), span_order)

    key_count = both.shape[0]
    key_rows = both[:, :kv_width].reshape(key_count, kv_heads, HEAD_SIZE)
    value_rows = both[:, kv_width:].reshape(key_count, kv_heads, HEAD_SIZE)
    shaped_queries = queries.reshape(tok_rows, kv_heads, head_cluster, HEAD_SIZE)
    scores = jnp.einsum("qhgd,khd->hgqk", shaped_queries, key_rows, preferred_element_type=f32)
    allowed = key_pos[None, :] <= query_pos[:, None]
    scores = jnp.where(allowed[None, None], scores * (1.0 / math.sqrt(HEAD_SIZE)), -1e30)
    peak = jnp.max(scores, axis=-1)
    weights = jnp.where(allowed[None, None], jnp.exp(scores - peak[..., None]), 0.0)
    denominator = jnp.sum(weights, axis=-1)
    weighted = jnp.einsum("hgqk,khd->qhgd", weights.astype(bf16), value_rows, preferred_element_type=f32)
    attended = (
        (weighted / jnp.transpose(denominator, (2, 0, 1))[..., None]).astype(bf16).reshape(tok_rows, -1)
    )

    sub = resid_in.shape[0]

    def projected(step):
        rows = lax.dynamic_slice_in_dim(attended, ((mine + step) % 4) * sub, sub, 0)
        return jnp.dot(rows, out_weight, preferred_element_type=f32)

    far_sum = shift_exp(projected(2).astype(bf16), 2)
    up_sum = shift_exp(projected(1).astype(bf16), 1)
    down_sum = shift_exp(projected(3).astype(bf16), 3)
    own_sum = (projected(0) + far_sum.astype(f32)) + (up_sum.astype(f32) + down_sum.astype(f32))
    stream = (resid_in.astype(f32) + own_sum).astype(bf16)
    stream_wide = stream.astype(f32)
    mean_square = jnp.mean(stream_wide * stream_wide, axis=-1, keepdims=True)
    normed = (stream_wide * lax.rsqrt(mean_square + 1e-05) * norm_gain).astype(bf16)
    logits = jnp.dot(normed.astype(f32), router, precision=lax.Precision.HIGHEST)
    experts = router.shape[1]
    expert_axis = (mine + jnp.arange(experts, dtype=jnp.int32)) % experts
    picked = expert_ids[:, :, None] == jnp.arange(experts, dtype=jnp.int32)[None, None, :]
    chosen = jnp.sum(jnp.where(picked, logits[:, None, :], 0.0), axis=-1)
    mixing = jax.nn.softmax(chosen, axis=-1)
    picked = expert_ids[:, :, None] == expert_axis[None, None, :]
    token_weight = jnp.sum(jnp.where(picked, mixing[:, :, None], 0.0), axis=1)
    routed = jnp.any(picked, axis=1)
    rank_of = jnp.cumsum(routed.astype(jnp.int32), axis=0) - 1
    slot_count = sub * expert_ids.shape[1] // experts
    slot_axis = jnp.arange(slot_count, dtype=jnp.int32)
    placing = jnp.logical_and(routed.T[:, None, :], rank_of.T[:, None, :] == slot_axis[None, :, None])
    outgoing = jnp.dot(
        placing.reshape(experts * slot_count, sub).astype(bf16), normed, preferred_element_type=f32
    ).astype(bf16)
    o0, o1, o2, o3 = quarters(outgoing)
    rows = join(o0, shift_exp(o1, 1), shift_exp(o2, 2), shift_exp(o3, 3))

    gate_b, up_b, down_b = swap(w_gate[0]), swap(w_up[0]), swap(w_down[0])

    def expert(a):
        def hidden(gate, up):
            g = jnp.dot(a, gate, preferred_element_type=f32)
            u = jnp.dot(a, up, preferred_element_type=f32)
            return (jax.nn.silu(g) * u).astype(bf16)

        return (
            jnp.dot(hidden(w_gate[0], w_up[0]), w_down[0], preferred_element_type=f32)
            + jnp.dot(hidden(gate_b, up_b), down_b, preferred_element_type=f32)
        ).astype(bf16)

    near_rows = gather_ring(rows, 1)
    side_rows, far_rows = gather_ring_split(near_rows, 2)
    near_out = expert(near_rows)
    side_out = expert(side_rows)
    far_out = expert(far_rows)
    block = near_out.shape[0]
    part = sum_ring_split(near_out, side_out[:block], side_out[block:], far_out, 2)
    own_rows = sum_ring(*quarters(part), 1).astype(bf16)

    r0, r1, r2, r3 = quarters(own_rows)
    returned = join(r0, shift_exp(r1, 3), shift_exp(r2, 2), shift_exp(r3, 1))
    coefficient = placing.astype(f32) * token_weight.T[:, None, :]
    combined = jnp.einsum("est,esd->td", coefficient, returned.reshape(experts, slot_count, -1).astype(f32))
    return (stream_wide + combined).astype(bf16)


def solution(mesh):
    placed = (
        P("ctx", "exp"),
        P("ctx", "exp"),
        P("ctx", "exp"),
        P(("ctx", "exp"), None),
        P(),
        P("exp", None),
        P(),
        P(),
        P(("ctx", "exp"), None),
        P("exp", None, "ctx"),
        P("exp", None, "ctx"),
        P("exp", "ctx", None),
    )
    return jax.shard_map(
        on_device, mesh=mesh, in_specs=placed, out_specs=P(("ctx", "exp"), None), check_vma=False
    )
```

```python
import math

import jax
import jax.numpy as jnp
from jax import lax
from jax.experimental import pallas as pl
from jax.experimental.pallas import tpu as pltpu
from jax.sharding import PartitionSpec as P

HEAD_SIZE = 128
SPAN = 64
RING = 4
NEVER = -1e30

f32 = jnp.float32
bf16 = jnp.bfloat16
i32 = jnp.int32


def ctx_index_of(z, x, core):
    return (z % RING) * 8 + (x % RING) * 2 + core


def ring_pairs(phase, step):
    pairs = []
    for z in range(RING):
        for x in range(RING):
            for core in range(2):
                along_x = (core == 0) == (phase == 1)
                target = ctx_index_of(z, x + step, core) if along_x else ctx_index_of(z + step, x, core)
                pairs.append((ctx_index_of(z, x, core), target))
    return pairs


RINGS = {(phase, step): ring_pairs(phase, step) for phase in (1, 2) for step in (1, -1, 2)}
SWAP = [(i, i ^ 1) for i in range(32)]


def shift(a, phase, step):
    return lax.ppermute(a, "ctx", RINGS[phase, step])


def swap(a):
    return lax.ppermute(a, "ctx", SWAP)


def shift_exp(a, step):
    return lax.ppermute(a, "exp", [(i, (i + step) % 4) for i in range(4)])


def join(*parts):
    return jnp.concatenate(parts, axis=0)


def total(*terms):
    return sum(t.astype(f32) for t in terms).astype(bf16)


def positions_of(span_ids, span_order):
    matches = span_ids[:, None] == jnp.arange(span_order.shape[0], dtype=i32)[None, :]
    starts = jnp.sum(jnp.where(matches, span_order[None, :], 0), axis=1) * SPAN
    return (starts[:, None] + jnp.arange(SPAN, dtype=i32)[None, :]).reshape(-1)


def attend_blocks(q_ref, qpos_ref, kpos_ref, kv_refs, first, m_ref, l_ref, acc_ref):
    tok = q_ref.shape[0]
    kv_heads = kv_refs[0].shape[1] // (2 * HEAD_SIZE)
    cluster = q_ref.shape[1] // HEAD_SIZE // kv_heads
    rows = cluster * tok
    slope = math.log2(math.e) / math.sqrt(HEAD_SIZE)
    masks = []
    for n, kv in enumerate(kv_refs):
        keep = kpos_ref[n : n + 1, :] <= qpos_ref[:, 0:1]
        masks.append(jnp.where(keep, 0.0, NEVER))
    for h in range(kv_heads):
        q = jnp.concatenate(
            [q_ref[:, (h * cluster + g) * HEAD_SIZE : (h * cluster + g + 1) * HEAD_SIZE] for g in range(cluster)],
            axis=0,
        )
        at = pl.ds(h * rows, rows)
        if not first:
            m, l, acc = m_ref[at, 0:1], l_ref[at, 0:1], acc_ref[at, :]
        for n, kv in enumerate(kv_refs):
            k = kv[:, h * HEAD_SIZE : (h + 1) * HEAD_SIZE]
            v = kv[:, (kv_heads + h) * HEAD_SIZE : (kv_heads + h + 1) * HEAD_SIZE]
            s = lax.dot_general(q, k, (((1,), (1,)), ((), ())), preferred_element_type=f32)
            s = (s.reshape(cluster, tok, -1) * slope + masks[n][None]).reshape(rows, -1)
            top = jnp.max(s, axis=1, keepdims=True)
            if first and n == 0:
                m = top
                p = jnp.exp2(s - m)
                l = jnp.sum(p, axis=1, keepdims=True)
                acc = jnp.dot(p.astype(bf16), v, preferred_element_type=f32)
            else:
                new = jnp.maximum(m, top)
                fade = jnp.exp2(m - new)
                p = jnp.exp2(s - new)
                l = l * fade + jnp.sum(p, axis=1, keepdims=True)
                acc = acc * fade + jnp.dot(p.astype(bf16), v, preferred_element_type=f32)
                m = new
        m_ref[at, :] = jnp.broadcast_to(m, (rows, HEAD_SIZE))
        l_ref[at, :] = jnp.broadcast_to(l, (rows, HEAD_SIZE))
        acc_ref[at, :] = acc


def vmem_spec():
    return pl.BlockSpec(memory_space=pltpu.VMEM)


def attend_cost(q, kvs):
    work = q.shape[0] * q.shape[1] * sum(kv.shape[0] for kv in kvs)
    return pl.CostEstimate(flops=8 * work, transcendentals=work // HEAD_SIZE, bytes_accessed=4 << 20)


def attend_part(q, qpos, kpos, kvs, state):
    heads = q.shape[1] // HEAD_SIZE
    rows = heads * q.shape[0]
    first = state is None

    def kernel(*refs):
        q_ref, qpos_ref, kpos_ref = refs[:3]
        kv_refs = refs[3 : 3 + len(kvs)]
        m_ref, l_ref, acc_ref = refs[-3:]
        if not first:
            old = refs[3 + len(kvs) : 6 + len(kvs)]
            for new, was in zip((m_ref, l_ref, acc_ref), old):
                new[...] = was[...]
        attend_blocks(q_ref, qpos_ref, kpos_ref, kv_refs, first, m_ref, l_ref, acc_ref)

    operands = (q, qpos, kpos, *kvs) + (() if first else tuple(state))
    shape = jax.ShapeDtypeStruct((rows, HEAD_SIZE), f32)
    return pl.pallas_call(
        kernel,
        out_shape=(shape, shape, shape),
        in_specs=[vmem_spec()] * len(operands),
        out_specs=(vmem_spec(),) * 3,
        cost_estimate=attend_cost(q, kvs),
        compiler_params=pltpu.CompilerParams(vmem_limit_bytes=40 << 20),
        name="attend_part",
    )(*operands)


def attend_last(mine, q, qpos, kpos, kvs, state, out_weight):
    tok = q.shape[0]
    heads = q.shape[1] // HEAD_SIZE
    rows = heads * tok
    sub = tok // 4
    width = out_weight.shape[1]

    def kernel(mine_ref, *refs):
        q_ref, qpos_ref, kpos_ref = refs[:3]
        kv_refs = refs[3 : 3 + len(kvs)]
        old = refs[3 + len(kvs) : 6 + len(kvs)]
        weight_hbm = refs[6 + len(kvs)]
        outs = refs[7 + len(kvs) : 11 + len(kvs)]
        m_ref, l_ref, acc_ref, weight, attended, ordered, sem = refs[11 + len(kvs) :]
        fetch = pltpu.make_async_copy(weight_hbm, weight, sem)
        fetch.start()
        for new, was in zip((m_ref, l_ref, acc_ref), old):
            new[...] = was[...]
        attend_blocks(q_ref, qpos_ref, kpos_ref, kv_refs, False, m_ref, l_ref, acc_ref)
        for h in range(heads):
            at = pl.ds(h * tok, tok)
            attended[:, h * HEAD_SIZE : (h + 1) * HEAD_SIZE] = (acc_ref[at, :] / l_ref[at, :]).astype(bf16)
        for r in range(4):
            start = pl.multiple_of(lax.rem(mine_ref[0] + r, 4) * sub, sub)
            ordered[r * sub : (r + 1) * sub, :] = attended[pl.ds(start, sub), :]
        fetch.wait()
        for n in range(4):
            at = pl.ds(n * (width // 4), width // 4)
            product = jnp.dot(ordered[...], weight[:, at], preferred_element_type=f32)
            for r in range(4):
                outs[r][:, at] = product[r * sub : (r + 1) * sub].astype(outs[r].dtype)

    operands = (q, qpos, kpos, *kvs, *state)
    return pl.pallas_call(
        kernel,
        out_shape=tuple(jax.ShapeDtypeStruct((sub, width), t) for t in (f32, bf16, bf16, bf16)),
        in_specs=[pl.BlockSpec(memory_space=pltpu.SMEM)]
        + [vmem_spec()] * len(operands)
        + [pl.BlockSpec(memory_space=pl.ANY)],
        out_specs=(vmem_spec(),) * 4,
        scratch_shapes=[
            pltpu.VMEM((rows, HEAD_SIZE), f32),
            pltpu.VMEM((rows, HEAD_SIZE), f32),
            pltpu.VMEM((rows, HEAD_SIZE), f32),
            pltpu.VMEM(out_weight.shape, bf16),
            pltpu.VMEM((tok, q.shape[1]), bf16),
            pltpu.VMEM((tok, q.shape[1]), bf16),
            pltpu.SemaphoreType.DMA,
        ],
        cost_estimate=attend_cost(q, kvs),
        compiler_params=pltpu.CompilerParams(vmem_limit_bytes=40 << 20),
        name="attend_last",
    )(mine, *operands, out_weight)


def expert_rows(pieces, own, other):
    depth, hid = own[0].shape
    width = own[2].shape[1]
    steps = 4
    deep, wide = depth // steps, width // steps
    sizes = [p.shape[0] for p in pieces]
    rows = sum(sizes)
    count = len(pieces)
    starts = [sum(sizes[:i]) for i in range(count)]

    def kernel(*refs):
        ins, refs = refs[:count], refs[count:]
        (ga, ua, da, gb, ub, db), refs = refs[:6], refs[6:]
        outs, refs = refs[:count], refs[count:]
        x, sums, hidden = refs
        step = pl.program_id(0)

        @pl.when(step < steps)
        def _():
            for ref, start, size in zip(ins, starts, sizes):
                x[start : start + size, :] = ref[...]
            for i, w in enumerate((ga, ua, gb, ub)):
                product = jnp.dot(x[...], w[...], preferred_element_type=f32)

                @pl.when(step == 0)
                def _():
                    sums[i] = product

                @pl.when(step > 0)
                def _():
                    sums[i] += product

        @pl.when(step == steps - 1)
        def _():
            for i in range(2):
                hidden[i] = (jax.nn.silu(sums[2 * i]) * sums[2 * i + 1]).astype(bf16)

        @pl.when(step >= steps)
        def _():
            product = jnp.dot(hidden[0], da[...], preferred_element_type=f32)
            product += jnp.dot(hidden[1], db[...], preferred_element_type=f32)
            for ref, start, size in zip(outs, starts, sizes):
                ref[...] = product[start : start + size].astype(bf16)

    def early(s):
        return jnp.minimum(s, steps - 1)

    def late(s):
        return jnp.maximum(s - steps, 0)

    tall = pl.BlockSpec((deep, hid), lambda s: (early(s), 0))
    flat = pl.BlockSpec((hid, wide), lambda s: (0, late(s)))
    return pl.pallas_call(
        kernel,
        grid=(2 * steps,),
        out_shape=tuple(jax.ShapeDtypeStruct((size, width), bf16) for size in sizes),
        in_specs=[pl.BlockSpec((size, deep), lambda s: (0, early(s))) for size in sizes]
        + [tall, tall, flat, tall, tall, flat],
        out_specs=tuple(pl.BlockSpec((size, wide), lambda s: (0, late(s))) for size in sizes),
        scratch_shapes=[
            pltpu.VMEM((rows, deep), bf16),
            pltpu.VMEM((4, rows, hid), f32),
            pltpu.VMEM((2, rows, hid), bf16),
        ],
        cost_estimate=pl.CostEstimate(
            flops=12 * rows * depth * hid, transcendentals=2 * rows * hid, bytes_accessed=12 * depth * hid
        ),
        compiler_params=pltpu.CompilerParams(
            dimension_semantics=("arbitrary",), vmem_limit_bytes=40 << 20
        ),
        name="expert_rows",
    )(*pieces, own[0], own[1], own[2], other[0], other[1], other[2])


def on_device(
    queries,
    keys,
    values,
    resid_in,
    span_order,
    out_weight,
    norm_gain,
    router,
    expert_ids,
    w_gate,
    w_up,
    w_down,
):
    me = lax.axis_index("ctx")
    mine = lax.axis_index("exp").astype(i32)
    my_z, my_x, my_core = me // 8, (me // 2) % RING, me % 2

    kv = jnp.concatenate((keys, values), axis=1)
    near = join(kv, shift(kv, 1, 1), shift(kv, 1, -1), shift(kv, 1, 2))
    left, right, far = shift(near, 2, 1), shift(near, 2, -1), shift(near, 2, 2)

    def block_positions(seconds):
        spans = []
        for second in seconds:
            for core in (my_core, 1 - my_core):
                a = jnp.array([0, -1, 1, 2], i32)
                z = jnp.where(core == 0, my_z + second, my_z + a) % RING
                x = jnp.where(core == 0, my_x + a, my_x + second) % RING
                block = z * 8 + x * 2 + core
                spans.append((block[:, None] * 2 + jnp.arange(2, dtype=i32)[None, :]).reshape(-1))
        return positions_of(jnp.concatenate(spans), span_order).reshape(2 * len(seconds), -1)

    query_pos = positions_of(me * 2 + jnp.arange(2, dtype=i32), span_order)
    query_pos = jnp.broadcast_to(query_pos[:, None], (query_pos.shape[0], HEAD_SIZE))
    state = attend_part(queries, query_pos, block_positions((0,)), (near, swap(near)), None)
    state = attend_part(
        queries, query_pos, block_positions((-1, 1)), (left, swap(left), right, swap(right)), state
    )
    sum0, sum1, sum2, sum3 = attend_last(
        mine.reshape(1), queries, query_pos, block_positions((2,)), (far, swap(far)), state, out_weight
    )

    sub = resid_in.shape[0]
    back2, back1, back3 = shift_exp(sum2, 2), shift_exp(sum1, 1), shift_exp(sum3, 3)
    own_sum = (sum0 + back2.astype(f32)) + (back1.astype(f32) + back3.astype(f32))
    stream = (resid_in.astype(f32) + own_sum).astype(bf16)
    stream_wide = stream.astype(f32)
    mean_square = jnp.mean(stream_wide * stream_wide, axis=-1, keepdims=True)
    normed = (stream_wide * lax.rsqrt(mean_square + 1e-05) * norm_gain).astype(bf16)
    logits = jnp.dot(normed.astype(f32), router, precision=lax.Precision.HIGHEST)
    experts = router.shape[1]
    expert_axis = (mine + jnp.arange(experts, dtype=i32)) % experts
    picked = expert_ids[:, :, None] == jnp.arange(experts, dtype=i32)[None, None, :]
    chosen = jnp.sum(jnp.where(picked, logits[:, None, :], 0.0), axis=-1)
    mixing = jax.nn.softmax(chosen, axis=-1)
    picked = expert_ids[:, :, None] == expert_axis[None, None, :]
    token_weight = jnp.sum(jnp.where(picked, mixing[:, :, None], 0.0), axis=1)
    routed = jnp.any(picked, axis=1)
    rank_of = jnp.cumsum(routed.astype(i32), axis=0) - 1
    slot_count = sub * expert_ids.shape[1] // experts
    slot_axis = jnp.arange(slot_count, dtype=i32)
    placing = jnp.logical_and(routed.T[:, None, :], rank_of.T[:, None, :] == slot_axis[None, :, None])
    outgoing = jnp.dot(
        placing.reshape(experts * slot_count, sub).astype(bf16), normed, preferred_element_type=f32
    ).astype(bf16)
    o0, o1, o2, o3 = (outgoing[i * slot_count : (i + 1) * slot_count] for i in range(4))
    rows = join(o0, shift_exp(o1, 1), shift_exp(o2, 2), shift_exp(o3, 3))

    own = (w_gate[0], w_up[0], w_down[0])
    other = tuple(swap(w) for w in own)
    n0 = join(rows, shift(rows, 1, 1))
    n1 = join(shift(rows, 1, -1), shift(rows, 1, 2))
    l0, r0 = shift(n0, 2, 1), shift(n0, 2, -1)
    r1, l1 = shift(n1, 2, -1), shift(n1, 2, 1)
    f0, f1 = shift(l0, 2, 1), shift(r1, 2, -1)

    n0, n1 = expert_rows((n0, n1), own, other)
    l0, l1, r0, r1 = expert_rows((l0, l1, r0, r1), own, other)
    f0, f1 = expert_rows((f0, f1), own, other)

    u1, v0 = shift(l1, 2, -1), shift(r0, 2, 1)
    q0, q1 = shift(f0, 2, -1), shift(f1, 2, 1)
    u0, v1 = shift(total(l0, q0), 2, -1), shift(total(r1, q1), 2, 1)
    n0, n1 = total(n0, u0, v0), total(n1, u1, v1)
    part = rows.shape[0]
    back = (shift(n0[part:], 1, -1), shift(n1[:part], 1, 1), shift(n1[part:], 1, 2))
    own_rows = total(n0[:part], *back)

    r0, r1, r2, r3 = (own_rows[i * slot_count : (i + 1) * slot_count] for i in range(4))
    returned = join(r0, shift_exp(r1, 3), shift_exp(r2, 2), shift_exp(r3, 1))
    coefficient = placing.astype(f32) * token_weight.T[:, None, :]
    combined = jnp.einsum("est,esd->td", coefficient, returned.reshape(experts, slot_count, -1).astype(f32))
    return (stream_wide + combined).astype(bf16)


def solution(mesh):
    placed = (
        P("ctx", "exp"),
        P("ctx", "exp"),
        P("ctx", "exp"),
        P(("ctx", "exp"), None),
        P(),
        P("exp", None),
        P(),
        P(),
        P(("ctx", "exp"), None),
        P("exp", None, "ctx"),
        P("exp", None, "ctx"),
        P("exp", "ctx", None),
    )
    return jax.shard_map(
        on_device, mesh=mesh, in_specs=placed, out_specs=P(("ctx", "exp"), None), check_vma=False
    )
```

```python
import math

import jax
import jax.numpy as jnp
from jax import lax
from jax.experimental import pallas as pl
from jax.experimental.pallas import tpu as pltpu
from jax.sharding import PartitionSpec as P

HEAD_SIZE = 128
SPAN = 64
RING = 4
NEVER = -1e30

f32 = jnp.float32
bf16 = jnp.bfloat16
i32 = jnp.int32


def ctx_index_of(z, x, core):
    return (z % RING) * 8 + (x % RING) * 2 + core


def ring_pairs(phase, step):
    pairs = []
    for z in range(RING):
        for x in range(RING):
            for core in range(2):
                along_x = (core == 0) == (phase == 1)
                target = ctx_index_of(z, x + step, core) if along_x else ctx_index_of(z + step, x, core)
                pairs.append((ctx_index_of(z, x, core), target))
    return pairs


RINGS = {(phase, step): ring_pairs(phase, step) for phase in (1, 2) for step in (1, -1, 2)}
SWAP = [(i, i ^ 1) for i in range(32)]


def shift(a, phase, step):
    return lax.ppermute(a, "ctx", RINGS[phase, step])


def swap(a):
    return lax.ppermute(a, "ctx", SWAP)


def shift_exp(a, step):
    return lax.ppermute(a, "exp", [(i, (i + step) % 4) for i in range(4)])


def join(*parts):
    return jnp.concatenate(parts, axis=0)


def total(*terms):
    return sum(t.astype(f32) for t in terms).astype(bf16)


def positions_of(span_ids, span_order):
    matches = span_ids[:, None] == jnp.arange(span_order.shape[0], dtype=i32)[None, :]
    starts = jnp.sum(jnp.where(matches, span_order[None, :], 0), axis=1) * SPAN
    return (starts[:, None] + jnp.arange(SPAN, dtype=i32)[None, :]).reshape(-1)


def attend_blocks(q_ref, qpos_ref, kpos_ref, kv_refs, old, m_ref, l_ref, acc_ref):
    tok = q_ref.shape[0]
    kv_heads = kv_refs[0].shape[1] // (2 * HEAD_SIZE)
    cluster = q_ref.shape[1] // HEAD_SIZE // kv_heads
    rows = cluster * tok
    slope = math.log2(math.e) / math.sqrt(HEAD_SIZE)
    masks = []
    for n, kv in enumerate(kv_refs):
        keep = kpos_ref[n : n + 1, :] <= qpos_ref[:, 0:1]
        masks.append(jnp.where(keep, 0.0, NEVER))
    for h in range(kv_heads):
        q = jnp.concatenate(
            [q_ref[:, (h * cluster + g) * HEAD_SIZE : (h * cluster + g + 1) * HEAD_SIZE] for g in range(cluster)],
            axis=0,
        )
        at = pl.ds(h * rows, rows)
        if old is not None:
            m = jnp.max(old[0][at, :], axis=1, keepdims=True)
            l = jnp.max(old[1][at, :], axis=1, keepdims=True)
            acc = old[2][at, :]
        for n, kv in enumerate(kv_refs):
            k = kv[:, h * HEAD_SIZE : (h + 1) * HEAD_SIZE]
            v = kv[:, (kv_heads + h) * HEAD_SIZE : (kv_heads + h + 1) * HEAD_SIZE]
            s = lax.dot_general(q, k, (((1,), (1,)), ((), ())), preferred_element_type=f32)
            s = (s.reshape(cluster, tok, -1) * slope + masks[n][None]).reshape(rows, -1)
            top = jnp.max(s, axis=1, keepdims=True)
            if old is None and n == 0:
                m = top
                p = jnp.exp2(s - m)
                l = jnp.sum(p, axis=1, keepdims=True)
                acc = jnp.dot(p.astype(bf16), v, preferred_element_type=f32)
            else:
                new = jnp.maximum(m, top)
                fade = jnp.exp2(m - new)
                p = jnp.exp2(s - new)
                l = l * fade + jnp.sum(p, axis=1, keepdims=True)
                acc = acc * fade + jnp.dot(p.astype(bf16), v, preferred_element_type=f32)
                m = new
        m_ref[at, :] = jnp.broadcast_to(m, (rows, HEAD_SIZE))
        l_ref[at, :] = jnp.broadcast_to(l, (rows, HEAD_SIZE))
        acc_ref[at, :] = acc


def vmem_spec():
    return pl.BlockSpec(memory_space=pltpu.VMEM)


def attend_cost(q, kvs):
    work = q.shape[0] * q.shape[1] * sum(kv.shape[0] for kv in kvs)
    return pl.CostEstimate(flops=8 * work, transcendentals=work // HEAD_SIZE, bytes_accessed=4 << 20)


def attend_part(q, qpos, kpos, kvs, state):
    heads = q.shape[1] // HEAD_SIZE
    rows = heads * q.shape[0]
    first = state is None

    def kernel(*refs):
        q_ref, qpos_ref, kpos_ref = refs[:3]
        kv_refs = refs[3 : 3 + len(kvs)]
        m_ref, l_ref, acc_ref = refs[-3:]
        old = None if first else refs[3 + len(kvs) : 6 + len(kvs)]
        attend_blocks(q_ref, qpos_ref, kpos_ref, kv_refs, old, m_ref, l_ref, acc_ref)

    operands = (q, qpos, kpos, *kvs) + (() if first else tuple(state))
    shape = jax.ShapeDtypeStruct((rows, HEAD_SIZE), f32)
    return pl.pallas_call(
        kernel,
        out_shape=(shape, shape, shape),
        in_specs=[vmem_spec()] * len(operands),
        out_specs=(vmem_spec(),) * 3,
        cost_estimate=attend_cost(q, kvs),
        compiler_params=pltpu.CompilerParams(vmem_limit_bytes=40 << 20),
        name="attend_part",
    )(*operands)


def attend_last(mine, q, qpos, kpos, kvs, state, out_weight):
    tok = q.shape[0]
    heads = q.shape[1] // HEAD_SIZE
    rows = heads * tok
    sub = tok // 4
    width = out_weight.shape[1]

    def kernel(mine_ref, *refs):
        q_ref, qpos_ref, kpos_ref = refs[:3]
        kv_refs = refs[3 : 3 + len(kvs)]
        old = refs[3 + len(kvs) : 6 + len(kvs)]
        weight_hbm = refs[6 + len(kvs)]
        outs = refs[7 + len(kvs) : 11 + len(kvs)]
        m_ref, l_ref, acc_ref, weight, attended, ordered, sem = refs[11 + len(kvs) :]
        fetch = pltpu.make_async_copy(weight_hbm, weight, sem)
        fetch.start()
        attend_blocks(q_ref, qpos_ref, kpos_ref, kv_refs, old, m_ref, l_ref, acc_ref)
        for h in range(heads):
            at = pl.ds(h * tok, tok)
            attended[:, h * HEAD_SIZE : (h + 1) * HEAD_SIZE] = (acc_ref[at, :] / l_ref[at, :]).astype(bf16)
        for r in range(4):
            start = pl.multiple_of(lax.rem(mine_ref[0] + r, 4) * sub, sub)
            ordered[r * sub : (r + 1) * sub, :] = attended[pl.ds(start, sub), :]
        fetch.wait()
        for n in range(4):
            at = pl.ds(n * (width // 4), width // 4)
            product = jnp.dot(ordered[...], weight[:, at], preferred_element_type=f32)
            for r in range(4):
                outs[r][:, at] = product[r * sub : (r + 1) * sub].astype(outs[r].dtype)

    operands = (q, qpos, kpos, *kvs, *state)
    return pl.pallas_call(
        kernel,
        out_shape=tuple(jax.ShapeDtypeStruct((sub, width), t) for t in (f32, bf16, bf16, bf16)),
        in_specs=[pl.BlockSpec(memory_space=pltpu.SMEM)]
        + [vmem_spec()] * len(operands)
        + [pl.BlockSpec(memory_space=pl.ANY)],
        out_specs=(vmem_spec(),) * 4,
        scratch_shapes=[
            pltpu.VMEM((rows, HEAD_SIZE), f32),
            pltpu.VMEM((rows, HEAD_SIZE), f32),
            pltpu.VMEM((rows, HEAD_SIZE), f32),
            pltpu.VMEM(out_weight.shape, bf16),
            pltpu.VMEM((tok, q.shape[1]), bf16),
            pltpu.VMEM((tok, q.shape[1]), bf16),
            pltpu.SemaphoreType.DMA,
        ],
        cost_estimate=attend_cost(q, kvs),
        compiler_params=pltpu.CompilerParams(vmem_limit_bytes=40 << 20),
        name="attend_last",
    )(mine, *operands, out_weight)


def expert_rows(pieces, own, other):
    hid, depth = own[0].shape
    width = own[2].shape[1]
    chunks = 4
    deep, wide = depth // chunks, width // chunks
    sizes = [p.shape[0] for p in pieces]
    rows = sum(sizes)
    count = len(pieces)
    starts = [sum(sizes[:i]) for i in range(count)]

    def kernel(*refs):
        ins, refs = refs[:count], refs[count:]
        (ga, ua, da, gb, ub, db), refs = refs[:6], refs[6:]
        outs, refs = refs[:count], refs[count:]
        x, w, dw, sums, hidden, out, x_sems, w_sems, d_sems, out_sems = refs

        def first_copies(k):
            at = pl.ds(pl.multiple_of(k * deep, deep), deep)
            for i, ref in enumerate((ga, gb, ua, ub)):
                yield pltpu.make_async_copy(ref.at[:, at], w.at[k, pl.ds(i * hid, hid), :], w_sems.at[k, i])
            for i, ref in enumerate(ins):
                yield pltpu.make_async_copy(
                    ref.at[:, at], x.at[k, pl.ds(starts[i], sizes[i]), :], x_sems.at[k, i]
                )

        def last_copies(n):
            at = pl.ds(pl.multiple_of(n * wide, wide), wide)
            for i, ref in enumerate((da, db)):
                yield pltpu.make_async_copy(ref.at[:, at], dw.at[n, pl.ds(i * hid, hid), :], d_sems.at[n, i])

        def out_copies(n):
            at = pl.ds(pl.multiple_of(n * wide, wide), wide)
            for i, ref in enumerate(outs):
                yield pltpu.make_async_copy(
                    out.at[n, pl.ds(starts[i], sizes[i]), :], ref.at[:, at], out_sems.at[n, i]
                )

        for k in range(chunks):
            for copy in first_copies(k):
                copy.start()
        for n in range(chunks):
            for copy in last_copies(n):
                copy.start()
        sums[...] = jnp.zeros_like(sums)

        @pl.loop(0, chunks)
        def _(k):
            for copy in first_copies(k):
                copy.wait()
            sums[...] += lax.dot_general(x[k], w[k], (((1,), (1,)), ((), ())), preferred_element_type=f32)

        hidden[...] = (jax.nn.silu(sums[:, : 2 * hid]) * sums[:, 2 * hid :]).astype(bf16)

        @pl.loop(0, chunks)
        def _(n):
            for copy in last_copies(n):
                copy.wait()
            out[n] = jnp.dot(hidden[...], dw[n], preferred_element_type=f32).astype(bf16)
            for copy in out_copies(n):
                copy.start()

        for n in range(chunks):
            for copy in out_copies(n):
                copy.wait()

    anywhere = pl.BlockSpec(memory_space=pl.ANY)
    return pl.pallas_call(
        kernel,
        out_shape=tuple(jax.ShapeDtypeStruct((size, width), bf16) for size in sizes),
        in_specs=[anywhere] * (count + 6),
        out_specs=(anywhere,) * count,
        scratch_shapes=[
            pltpu.VMEM((chunks, rows, deep), bf16),
            pltpu.VMEM((chunks, 4 * hid, deep), bf16),
            pltpu.VMEM((chunks, 2 * hid, wide), bf16),
            pltpu.VMEM((rows, 4 * hid), f32),
            pltpu.VMEM((rows, 2 * hid), bf16),
            pltpu.VMEM((chunks, rows, wide), bf16),
            pltpu.SemaphoreType.DMA((chunks, count)),
            pltpu.SemaphoreType.DMA((chunks, 4)),
            pltpu.SemaphoreType.DMA((chunks, 2)),
            pltpu.SemaphoreType.DMA((chunks, count)),
        ],
        cost_estimate=pl.CostEstimate(
            flops=12 * rows * depth * hid, transcendentals=2 * rows * hid, bytes_accessed=12 * depth * hid
        ),
        compiler_params=pltpu.CompilerParams(vmem_limit_bytes=(26 << 20) + rows * (32 << 10)),
        name="expert_rows",
    )(*pieces, *own, *other)


def layer(
    queries,
    keys,
    values,
    resid_in,
    span_order,
    out_weight,
    norm_gain,
    router,
    expert_ids,
    w_gate,
    w_up,
    w_down,
):
    me = lax.axis_index("ctx")
    mine = lax.axis_index("exp").astype(i32)
    my_z, my_x, my_core = me // 8, (me // 2) % RING, me % 2

    kv = jnp.concatenate((keys, values), axis=1)
    near = join(kv, shift(kv, 1, 1), shift(kv, 1, -1), shift(kv, 1, 2))
    left, right = shift(near, 2, 1), shift(near, 2, -1)
    far = shift(near, 2, 2)

    def block_positions(seconds):
        spans = []
        for second in seconds:
            for core in (my_core, 1 - my_core):
                a = jnp.array([0, -1, 1, 2], i32)
                z = jnp.where(core == 0, my_z + second, my_z + a) % RING
                x = jnp.where(core == 0, my_x + a, my_x + second) % RING
                block = z * 8 + x * 2 + core
                spans.append((block[:, None] * 2 + jnp.arange(2, dtype=i32)[None, :]).reshape(-1))
        return positions_of(jnp.concatenate(spans), span_order).reshape(2 * len(seconds), -1)

    query_pos = positions_of(me * 2 + jnp.arange(2, dtype=i32), span_order)
    query_pos = jnp.broadcast_to(query_pos[:, None], (query_pos.shape[0], HEAD_SIZE))
    near_other, far_other = swap(near), swap(far)
    left_other, right_other = swap(left), swap(right)
    state = attend_part(queries, query_pos, block_positions((0,)), (near, near_other), None)
    state = attend_part(
        queries,
        query_pos,
        block_positions((-1, 1)),
        (left, left_other, right, right_other),
        state,
    )
    sum0, sum1, sum2, sum3 = attend_last(
        mine.reshape(1), queries, query_pos, block_positions((2,)), (far, far_other), state, out_weight
    )

    sub = resid_in.shape[0]
    back2, back1, back3 = shift_exp(sum2, 2), shift_exp(sum1, 1), shift_exp(sum3, 3)
    own_sum = (sum0 + back2.astype(f32)) + (back1.astype(f32) + back3.astype(f32))
    stream = (resid_in.astype(f32) + own_sum).astype(bf16)
    stream_wide = stream.astype(f32)
    mean_square = jnp.mean(stream_wide * stream_wide, axis=-1, keepdims=True)
    normed = (stream_wide * lax.rsqrt(mean_square + 1e-05) * norm_gain).astype(bf16)
    logits = jnp.dot(normed.astype(f32), router, precision=lax.Precision.HIGHEST)
    experts = router.shape[1]
    expert_axis = (mine + jnp.arange(experts, dtype=i32)) % experts
    picked = expert_ids[:, :, None] == jnp.arange(experts, dtype=i32)[None, None, :]
    chosen = jnp.sum(jnp.where(picked, logits[:, None, :], 0.0), axis=-1)
    mixing = jax.nn.softmax(chosen, axis=-1)
    picked = expert_ids[:, :, None] == expert_axis[None, None, :]
    token_weight = jnp.sum(jnp.where(picked, mixing[:, :, None], 0.0), axis=1)
    routed = jnp.any(picked, axis=1)
    rank_of = jnp.cumsum(routed.astype(i32), axis=0) - 1
    slot_count = sub * expert_ids.shape[1] // experts
    slot_axis = jnp.arange(slot_count, dtype=i32)
    placing = jnp.logical_and(routed.T[:, None, :], rank_of.T[:, None, :] == slot_axis[None, :, None])
    outgoing = jnp.dot(
        placing.reshape(experts * slot_count, sub).astype(bf16), normed, preferred_element_type=f32
    ).astype(bf16)
    o0, o1, o2, o3 = (outgoing[i * slot_count : (i + 1) * slot_count] for i in range(4))
    rows = join(o0, shift_exp(o1, 1), shift_exp(o2, 2), shift_exp(o3, 3))

    own = (w_gate[0].T, w_up[0].T, w_down[0])
    other = tuple(swap(w) for w in own)
    n0 = join(rows, shift(rows, 1, 1))
    n1 = join(shift(rows, 1, -1), shift(rows, 1, 2))
    l0, r0 = shift(n0, 2, 1), shift(n0, 2, -1)
    r1, l1 = shift(n1, 2, -1), shift(n1, 2, 1)
    f0, f1 = shift(l0, 2, 1), shift(r1, 2, -1)

    n0, n1 = expert_rows((n0, n1), own, other)
    l0, l1, r0, r1 = expert_rows((l0, l1, r0, r1), own, other)
    f0, f1 = expert_rows((f0, f1), own, other)

    u1, v0 = shift(l1, 2, -1), shift(r0, 2, 1)
    q0, q1 = shift(f0, 2, -1), shift(f1, 2, 1)
    u0, v1 = shift(total(l0, q0), 2, -1), shift(total(r1, q1), 2, 1)
    n0, n1 = total(n0, u0, v0), total(n1, u1, v1)
    part = rows.shape[0]
    back = (shift(n0[part:], 1, -1), shift(n1[:part], 1, 1), shift(n1[part:], 1, 2))
    own_rows = total(n0[:part], *back)

    r0, r1, r2, r3 = (own_rows[i * slot_count : (i + 1) * slot_count] for i in range(4))
    returned = join(r0, shift_exp(r1, 3), shift_exp(r2, 2), shift_exp(r3, 1))
    coefficient = placing.astype(f32) * token_weight.T[:, None, :]
    combined = jnp.einsum("est,esd->td", coefficient, returned.reshape(experts, slot_count, -1).astype(f32))
    return (stream_wide + combined).astype(bf16)


def solution(mesh):
    placed = (
        P("ctx", "exp"),
        P("ctx", "exp"),
        P("ctx", "exp"),
        P(("ctx", "exp"), None),
        P(),
        P("exp", None),
        P(),
        P(),
        P(("ctx", "exp"), None),
        P("exp", None, "ctx"),
        P("exp", None, "ctx"),
        P("exp", "ctx", None),
    )
    return jax.shard_map(layer, mesh=mesh, in_specs=placed, out_specs=P(("ctx", "exp"), None), check_vma=False)
```

```python
import math

import jax
import jax.numpy as jnp
from jax import lax
from jax.experimental import pallas as pl
from jax.experimental.pallas import tpu as pltpu
from jax.sharding import PartitionSpec as P

HEAD_SIZE = 128
SPAN = 64
RING = 4
NEVER = -1e30

f32 = jnp.float32
bf16 = jnp.bfloat16
i32 = jnp.int32


def ctx_index_of(z, x, core):
    return (z % RING) * 8 + (x % RING) * 2 + core


def ring_pairs(phase, step):
    pairs = []
    for z in range(RING):
        for x in range(RING):
            for core in range(2):
                along_x = (core == 0) == (phase == 1)
                target = ctx_index_of(z, x + step, core) if along_x else ctx_index_of(z + step, x, core)
                pairs.append((ctx_index_of(z, x, core), target))
    return pairs


RINGS = {(phase, step): ring_pairs(phase, step) for phase in (1, 2) for step in (1, -1, 2)}
SWAP = [(i, i ^ 1) for i in range(32)]


def shift(a, phase, step):
    return lax.ppermute(a, "ctx", RINGS[phase, step])


def swap(a):
    return lax.ppermute(a, "ctx", SWAP)


def shift_exp(a, step):
    return lax.ppermute(a, "exp", [(i, (i + step) % 4) for i in range(4)])


def join(*parts):
    return jnp.concatenate(parts, axis=0)


def total(*terms):
    return sum(t.astype(f32) for t in terms).astype(bf16)


def positions_of(span_ids, span_order):
    matches = span_ids[:, None] == jnp.arange(span_order.shape[0], dtype=i32)[None, :]
    starts = jnp.sum(jnp.where(matches, span_order[None, :], 0), axis=1) * SPAN
    return (starts[:, None] + jnp.arange(SPAN, dtype=i32)[None, :]).reshape(-1)


def attend_blocks(q_ref, qpos_ref, kpos_ref, kv_refs, old, m_ref, l_ref, acc_ref):
    tok = q_ref.shape[0]
    kv_heads = kv_refs[0].shape[1] // (2 * HEAD_SIZE)
    cluster = q_ref.shape[1] // HEAD_SIZE // kv_heads
    rows = cluster * tok
    slope = math.log2(math.e) / math.sqrt(HEAD_SIZE)
    masks = []
    for n, kv in enumerate(kv_refs):
        keep = kpos_ref[n : n + 1, :] <= qpos_ref[:, 0:1]
        masks.append(jnp.where(keep, 0.0, NEVER))
    for h in range(kv_heads):
        q = jnp.concatenate(
            [q_ref[:, (h * cluster + g) * HEAD_SIZE : (h * cluster + g + 1) * HEAD_SIZE] for g in range(cluster)],
            axis=0,
        )
        at = pl.ds(h * rows, rows)
        if old is not None:
            m = jnp.max(old[0][at, :], axis=1, keepdims=True)
            l = jnp.max(old[1][at, :], axis=1, keepdims=True)
            acc = old[2][at, :]
        for n, kv in enumerate(kv_refs):
            k = kv[:, h * HEAD_SIZE : (h + 1) * HEAD_SIZE]
            v = kv[:, (kv_heads + h) * HEAD_SIZE : (kv_heads + h + 1) * HEAD_SIZE]
            s = lax.dot_general(q, k, (((1,), (1,)), ((), ())), preferred_element_type=f32)
            s = (s.reshape(cluster, tok, -1) * slope + masks[n][None]).reshape(rows, -1)
            top = jnp.max(s, axis=1, keepdims=True)
            if old is None and n == 0:
                m = top
                p = jnp.exp2(s - m)
                l = jnp.sum(p, axis=1, keepdims=True)
                acc = jnp.dot(p.astype(bf16), v, preferred_element_type=f32)
            else:
                new = jnp.maximum(m, top)
                fade = jnp.exp2(m - new)
                p = jnp.exp2(s - new)
                l = l * fade + jnp.sum(p, axis=1, keepdims=True)
                acc = acc * fade + jnp.dot(p.astype(bf16), v, preferred_element_type=f32)
                m = new
        m_ref[at, :] = jnp.broadcast_to(m, (rows, HEAD_SIZE))
        l_ref[at, :] = jnp.broadcast_to(l, (rows, HEAD_SIZE))
        acc_ref[at, :] = acc


def vmem_spec():
    return pl.BlockSpec(memory_space=pltpu.VMEM)


def attend_cost(q, kvs):
    work = q.shape[0] * q.shape[1] * sum(kv.shape[0] for kv in kvs)
    return pl.CostEstimate(flops=8 * work, transcendentals=work // HEAD_SIZE, bytes_accessed=4 << 20)


def attend_part(q, qpos, kpos, kvs, state):
    heads = q.shape[1] // HEAD_SIZE
    rows = heads * q.shape[0]
    first = state is None

    def kernel(*refs):
        q_ref, qpos_ref, kpos_ref = refs[:3]
        kv_refs = refs[3 : 3 + len(kvs)]
        m_ref, l_ref, acc_ref = refs[-3:]
        old = None if first else refs[3 + len(kvs) : 6 + len(kvs)]
        attend_blocks(q_ref, qpos_ref, kpos_ref, kv_refs, old, m_ref, l_ref, acc_ref)

    operands = (q, qpos, kpos, *kvs) + (() if first else tuple(state))
    shape = jax.ShapeDtypeStruct((rows, HEAD_SIZE), f32)
    return pl.pallas_call(
        kernel,
        out_shape=(shape, shape, shape),
        in_specs=[vmem_spec()] * len(operands),
        out_specs=(vmem_spec(),) * 3,
        cost_estimate=attend_cost(q, kvs),
        compiler_params=pltpu.CompilerParams(vmem_limit_bytes=40 << 20),
        name="attend_part",
    )(*operands)


def attend_last(mine, q, qpos, kpos, kvs, state, out_weight):
    tok = q.shape[0]
    heads = q.shape[1] // HEAD_SIZE
    rows = heads * tok
    sub = tok // 4
    width = out_weight.shape[1]

    def kernel(mine_ref, *refs):
        q_ref, qpos_ref, kpos_ref = refs[:3]
        kv_refs = refs[3 : 3 + len(kvs)]
        old = refs[3 + len(kvs) : 6 + len(kvs)]
        weight_hbm = refs[6 + len(kvs)]
        outs = refs[7 + len(kvs) : 11 + len(kvs)]
        m_ref, l_ref, acc_ref, weight, attended, ordered, sem = refs[11 + len(kvs) :]
        fetch = pltpu.make_async_copy(weight_hbm, weight, sem)
        fetch.start()
        attend_blocks(q_ref, qpos_ref, kpos_ref, kv_refs, old, m_ref, l_ref, acc_ref)
        for h in range(heads):
            at = pl.ds(h * tok, tok)
            attended[:, h * HEAD_SIZE : (h + 1) * HEAD_SIZE] = (acc_ref[at, :] / l_ref[at, :]).astype(bf16)
        for r in range(4):
            start = pl.multiple_of(lax.rem(mine_ref[0] + r, 4) * sub, sub)
            ordered[r * sub : (r + 1) * sub, :] = attended[pl.ds(start, sub), :]
        fetch.wait()
        for n in range(4):
            at = pl.ds(n * (width // 4), width // 4)
            product = jnp.dot(ordered[...], weight[:, at], preferred_element_type=f32)
            for r in range(4):
                outs[r][:, at] = product[r * sub : (r + 1) * sub].astype(outs[r].dtype)

    operands = (q, qpos, kpos, *kvs, *state)
    return pl.pallas_call(
        kernel,
        out_shape=tuple(jax.ShapeDtypeStruct((sub, width), t) for t in (f32, bf16, bf16, bf16)),
        in_specs=[pl.BlockSpec(memory_space=pltpu.SMEM)]
        + [vmem_spec()] * len(operands)
        + [pl.BlockSpec(memory_space=pl.ANY)],
        out_specs=(vmem_spec(),) * 4,
        scratch_shapes=[
            pltpu.VMEM((rows, HEAD_SIZE), f32),
            pltpu.VMEM((rows, HEAD_SIZE), f32),
            pltpu.VMEM((rows, HEAD_SIZE), f32),
            pltpu.VMEM(out_weight.shape, bf16),
            pltpu.VMEM((tok, q.shape[1]), bf16),
            pltpu.VMEM((tok, q.shape[1]), bf16),
            pltpu.SemaphoreType.DMA,
        ],
        cost_estimate=attend_cost(q, kvs),
        compiler_params=pltpu.CompilerParams(vmem_limit_bytes=40 << 20),
        name="attend_last",
    )(mine, *operands, out_weight)


def expert_rows(pieces, own, other):
    hid, depth = own[0].shape
    width = own[2].shape[1]
    chunks = 4
    deep, wide = depth // chunks, width // chunks
    sizes = [p.shape[0] for p in pieces]
    rows = sum(sizes)
    count = len(pieces)
    starts = [sum(sizes[:i]) for i in range(count)]

    def kernel(*refs):
        ins, refs = refs[:count], refs[count:]
        (ga, ua, da, gb, ub, db), refs = refs[:6], refs[6:]
        outs, refs = refs[:count], refs[count:]
        x, w, dw, sums, hidden, out, x_sems, w_sems, d_sems, out_sems = refs

        def first_copies(k):
            at = pl.ds(pl.multiple_of(k * deep, deep), deep)
            for i, ref in enumerate((ga, gb, ua, ub)):
                yield pltpu.make_async_copy(ref.at[:, at], w.at[k, pl.ds(i * hid, hid), :], w_sems.at[k, i])
            for i, ref in enumerate(ins):
                yield pltpu.make_async_copy(
                    ref.at[:, at], x.at[k, pl.ds(starts[i], sizes[i]), :], x_sems.at[k, i]
                )

        def last_copies(n):
            at = pl.ds(pl.multiple_of(n * wide, wide), wide)
            for i, ref in enumerate((da, db)):
                yield pltpu.make_async_copy(ref.at[:, at], dw.at[n, pl.ds(i * hid, hid), :], d_sems.at[n, i])

        def out_copies(n):
            at = pl.ds(pl.multiple_of(n * wide, wide), wide)
            for i, ref in enumerate(outs):
                yield pltpu.make_async_copy(
                    out.at[n, pl.ds(starts[i], sizes[i]), :], ref.at[:, at], out_sems.at[n, i]
                )

        for k in range(chunks):
            for copy in first_copies(k):
                copy.start()
        for n in range(chunks):
            for copy in last_copies(n):
                copy.start()
        sums[...] = jnp.zeros_like(sums)

        @pl.loop(0, chunks)
        def _(k):
            for copy in first_copies(k):
                copy.wait()
            sums[...] += lax.dot_general(x[k], w[k], (((1,), (1,)), ((), ())), preferred_element_type=f32)

        hidden[...] = (jax.nn.silu(sums[:, : 2 * hid]) * sums[:, 2 * hid :]).astype(bf16)

        @pl.loop(0, chunks)
        def _(n):
            for copy in last_copies(n):
                copy.wait()
            out[n] = jnp.dot(hidden[...], dw[n], preferred_element_type=f32).astype(bf16)
            for copy in out_copies(n):
                copy.start()

        for n in range(chunks):
            for copy in out_copies(n):
                copy.wait()

    anywhere = pl.BlockSpec(memory_space=pltpu.HBM)
    return pl.pallas_call(
        kernel,
        out_shape=tuple(jax.ShapeDtypeStruct((size, width), bf16) for size in sizes),
        in_specs=[anywhere] * (count + 6),
        out_specs=(anywhere,) * count,
        scratch_shapes=[
            pltpu.VMEM((chunks, rows, deep), bf16),
            pltpu.VMEM((chunks, 4 * hid, deep), bf16),
            pltpu.VMEM((chunks, 2 * hid, wide), bf16),
            pltpu.VMEM((rows, 4 * hid), f32),
            pltpu.VMEM((rows, 2 * hid), bf16),
            pltpu.VMEM((chunks, rows, wide), bf16),
            pltpu.SemaphoreType.DMA((chunks, count)),
            pltpu.SemaphoreType.DMA((chunks, 4)),
            pltpu.SemaphoreType.DMA((chunks, 2)),
            pltpu.SemaphoreType.DMA((chunks, count)),
        ],
        cost_estimate=pl.CostEstimate(
            flops=12 * rows * depth * hid, transcendentals=2 * rows * hid, bytes_accessed=12 * depth * hid
        ),
        compiler_params=pltpu.CompilerParams(vmem_limit_bytes=(26 << 20) + rows * (32 << 10)),
        name="expert_rows",
    )(*pieces, *own, *other)


def layer(
    queries,
    keys,
    values,
    resid_in,
    span_order,
    out_weight,
    norm_gain,
    router,
    expert_ids,
    w_gate,
    w_up,
    w_down,
):
    me = lax.axis_index("ctx")
    mine = lax.axis_index("exp").astype(i32)
    my_z, my_x, my_core = me // 8, (me // 2) % RING, me % 2

    kv = jnp.concatenate((keys, values), axis=1)
    near = join(kv, shift(kv, 1, 1), shift(kv, 1, -1), shift(kv, 1, 2))
    left, right = shift(near, 2, 1), shift(near, 2, -1)
    far = shift(near, 2, 2)

    def block_positions(seconds):
        spans = []
        for second in seconds:
            for core in (my_core, 1 - my_core):
                a = jnp.array([0, -1, 1, 2], i32)
                z = jnp.where(core == 0, my_z + second, my_z + a) % RING
                x = jnp.where(core == 0, my_x + a, my_x + second) % RING
                block = z * 8 + x * 2 + core
                spans.append((block[:, None] * 2 + jnp.arange(2, dtype=i32)[None, :]).reshape(-1))
        return positions_of(jnp.concatenate(spans), span_order).reshape(2 * len(seconds), -1)

    query_pos = positions_of(me * 2 + jnp.arange(2, dtype=i32), span_order)
    query_pos = jnp.broadcast_to(query_pos[:, None], (query_pos.shape[0], HEAD_SIZE))
    near_other, far_other = swap(near), swap(far)
    left_other, right_other = swap(left), swap(right)
    state = attend_part(queries, query_pos, block_positions((0,)), (near, near_other), None)
    state = attend_part(
        queries,
        query_pos,
        block_positions((-1, 1)),
        (left, left_other, right, right_other),
        state,
    )
    sum0, sum1, sum2, sum3 = attend_last(
        mine.reshape(1), queries, query_pos, block_positions((2,)), (far, far_other), state, out_weight
    )

    sub = resid_in.shape[0]
    back2, back1, back3 = shift_exp(sum2, 2), shift_exp(sum1, 1), shift_exp(sum3, 3)
    own_sum = (sum0 + back2.astype(f32)) + (back1.astype(f32) + back3.astype(f32))
    stream = (resid_in.astype(f32) + own_sum).astype(bf16)
    stream_wide = stream.astype(f32)
    mean_square = jnp.mean(stream_wide * stream_wide, axis=-1, keepdims=True)
    normed = (stream_wide * lax.rsqrt(mean_square + 1e-05) * norm_gain).astype(bf16)
    logits = jnp.dot(normed.astype(f32), router, precision=lax.Precision.HIGHEST)
    experts = router.shape[1]
    expert_axis = (mine + jnp.arange(experts, dtype=i32)) % experts
    picked = expert_ids[:, :, None] == jnp.arange(experts, dtype=i32)[None, None, :]
    chosen = jnp.sum(jnp.where(picked, logits[:, None, :], 0.0), axis=-1)
    mixing = jax.nn.softmax(chosen, axis=-1)
    picked = expert_ids[:, :, None] == expert_axis[None, None, :]
    token_weight = jnp.sum(jnp.where(picked, mixing[:, :, None], 0.0), axis=1)
    routed = jnp.any(picked, axis=1)
    rank_of = jnp.cumsum(routed.astype(i32), axis=0) - 1
    slot_count = sub * expert_ids.shape[1] // experts
    slot_axis = jnp.arange(slot_count, dtype=i32)
    placing = jnp.logical_and(routed.T[:, None, :], rank_of.T[:, None, :] == slot_axis[None, :, None])
    outgoing = jnp.dot(
        placing.reshape(experts * slot_count, sub).astype(bf16), normed, preferred_element_type=f32
    ).astype(bf16)
    o0, o1, o2, o3 = (outgoing[i * slot_count : (i + 1) * slot_count] for i in range(4))
    rows = join(o0, shift_exp(o1, 1), shift_exp(o2, 2), shift_exp(o3, 3))

    own = (w_gate[0].T, w_up[0].T, w_down[0])
    other = tuple(swap(w) for w in own)
    n0 = join(rows, shift(rows, 1, 1))
    n1 = join(shift(rows, 1, -1), shift(rows, 1, 2))
    l0, r0 = shift(n0, 2, 1), shift(n0, 2, -1)
    r1, l1 = shift(n1, 2, -1), shift(n1, 2, 1)
    f0, f1 = shift(l0, 2, 1), shift(r1, 2, -1)

    n0, n1 = expert_rows((n0, n1), own, other)
    l0, r1 = expert_rows((l0, r1), own, other)
    l1, r0 = expert_rows((l1, r0), own, other)
    f0, f1 = expert_rows((f0, f1), own, other)

    u1, v0 = shift(l1, 2, -1), shift(r0, 2, 1)
    q0, q1 = shift(f0, 2, -1), shift(f1, 2, 1)
    u0, v1 = shift(total(l0, q0), 2, -1), shift(total(r1, q1), 2, 1)
    n0, n1 = total(n0, u0, v0), total(n1, u1, v1)
    part = rows.shape[0]
    back = (shift(n0[part:], 1, -1), shift(n1[:part], 1, 1), shift(n1[part:], 1, 2))
    own_rows = total(n0[:part], *back)

    r0, r1, r2, r3 = (own_rows[i * slot_count : (i + 1) * slot_count] for i in range(4))
    returned = join(r0, shift_exp(r1, 3), shift_exp(r2, 2), shift_exp(r3, 1))
    coefficient = placing.astype(f32) * token_weight.T[:, None, :]
    combined = jnp.einsum("est,esd->td", coefficient, returned.reshape(experts, slot_count, -1).astype(f32))
    return (stream_wide + combined).astype(bf16)


def solution(mesh):
    placed = (
        P("ctx", "exp"),
        P("ctx", "exp"),
        P("ctx", "exp"),
        P(("ctx", "exp"), None),
        P(),
        P("exp", None),
        P(),
        P(),
        P(("ctx", "exp"), None),
        P("exp", None, "ctx"),
        P("exp", None, "ctx"),
        P("exp", "ctx", None),
    )
    return jax.shard_map(layer, mesh=mesh, in_specs=placed, out_specs=P(("ctx", "exp"), None), check_vma=False)
```

```python
import math

import jax
import jax.numpy as jnp
from jax import lax
from jax.experimental import pallas as pl
from jax.experimental.pallas import tpu as pltpu
from jax.sharding import PartitionSpec as P

HEAD_SIZE = 128
SPAN = 64
RING = 4
NEVER = -1e30

f32 = jnp.float32
bf16 = jnp.bfloat16
i32 = jnp.int32


def ctx_index_of(z, x, core):
    return (z % RING) * 8 + (x % RING) * 2 + core


def ring_pairs(phase, step):
    pairs = []
    for z in range(RING):
        for x in range(RING):
            for core in range(2):
                along_x = (core == 0) == (phase == 1)
                target = ctx_index_of(z, x + step, core) if along_x else ctx_index_of(z + step, x, core)
                pairs.append((ctx_index_of(z, x, core), target))
    return pairs


RINGS = {(phase, step): ring_pairs(phase, step) for phase in (1, 2) for step in (1, -1, 2)}
SWAP = [(i, i ^ 1) for i in range(32)]


def shift(a, phase, step):
    return lax.ppermute(a, "ctx", RINGS[phase, step])


def swap(a):
    return lax.ppermute(a, "ctx", SWAP)


def shift_exp(a, step):
    return lax.ppermute(a, "exp", [(i, (i + step) % 4) for i in range(4)])


def join(*parts):
    return jnp.concatenate(parts, axis=0)


def total(*terms):
    return sum(t.astype(f32) for t in terms).astype(bf16)


def positions_of(span_ids, span_order):
    matches = span_ids[:, None] == jnp.arange(span_order.shape[0], dtype=i32)[None, :]
    starts = jnp.sum(jnp.where(matches, span_order[None, :], 0), axis=1) * SPAN
    return (starts[:, None] + jnp.arange(SPAN, dtype=i32)[None, :]).reshape(-1)


def vmem_spec():
    return pl.BlockSpec(memory_space=pltpu.VMEM)


def attend(mine, q, qpos, kpos, kvs, out_weight):
    tok = q.shape[0]
    heads = q.shape[1] // HEAD_SIZE
    kv_heads = kvs[0].shape[1] // (2 * HEAD_SIZE)
    cluster = heads // kv_heads
    rows = cluster * tok
    sub = tok // 4
    width = out_weight.shape[1]
    count = len(kvs)
    slope = math.log2(math.e) / math.sqrt(HEAD_SIZE)

    def kernel(mine_ref, q_ref, qpos_ref, kpos_ref, *refs):
        kv_refs, weight_hbm = refs[:count], refs[count]
        outs = refs[count + 1 : count + 5]
        attended, ordered, weight, sem = refs[count + 5 :]
        fetch = pltpu.make_async_copy(weight_hbm, weight, sem)
        fetch.start()

        @pl.loop(0, kv_heads)
        def _(h):
            def column(i):
                return pl.ds(pl.multiple_of(i * HEAD_SIZE, HEAD_SIZE), HEAD_SIZE)

            q_rows = jnp.concatenate([q_ref[:, column(h * cluster + g)] for g in range(cluster)], axis=0)
            for n, kv in enumerate(kv_refs):
                k = kv[:, column(h)]
                v = kv[:, column(kv_heads + h)]
                s = lax.dot_general(q_rows, k, (((1,), (1,)), ((), ())), preferred_element_type=f32)
                mask = jnp.where(kpos_ref[n : n + 1, :] <= qpos_ref[:, 0:1], 0.0, NEVER)
                s = (s.reshape(cluster, tok, -1) * slope + mask[None]).reshape(rows, -1)
                top = jnp.max(s, axis=1, keepdims=True)
                if n == 0:
                    m = top
                    p = jnp.exp2(s - m)
                    l = jnp.sum(p, axis=1, keepdims=True)
                    acc = jnp.dot(p.astype(bf16), v, preferred_element_type=f32)
                else:
                    new = jnp.maximum(m, top)
                    fade = jnp.exp2(m - new)
                    p = jnp.exp2(s - new)
                    l = l * fade + jnp.sum(p, axis=1, keepdims=True)
                    acc = acc * fade + jnp.dot(p.astype(bf16), v, preferred_element_type=f32)
                    m = new
            result = (acc / l).astype(bf16)
            for g in range(cluster):
                attended[:, column(h * cluster + g)] = result[g * tok : (g + 1) * tok]

        for r in range(4):
            start = pl.multiple_of(lax.rem(mine_ref[0] + r, 4) * sub, sub)
            ordered[r * sub : (r + 1) * sub, :] = attended[pl.ds(start, sub), :]
        fetch.wait()

        @pl.loop(0, 4)
        def _(n):
            at = pl.ds(pl.multiple_of(n * (width // 4), width // 4), width // 4)
            product = jnp.dot(ordered[...], weight[:, at], preferred_element_type=f32)
            for r in range(4):
                outs[r][:, at] = product[r * sub : (r + 1) * sub].astype(outs[r].dtype)

    work = q.shape[0] * q.shape[1] * sum(kv.shape[0] for kv in kvs)
    return pl.pallas_call(
        kernel,
        out_shape=tuple(jax.ShapeDtypeStruct((sub, width), t) for t in (f32, bf16, bf16, bf16)),
        in_specs=[pl.BlockSpec(memory_space=pltpu.SMEM)] + [vmem_spec()] * (count + 3)
        + [pl.BlockSpec(memory_space=pltpu.HBM)],
        out_specs=(vmem_spec(),) * 4,
        scratch_shapes=[
            pltpu.VMEM((tok, q.shape[1]), bf16),
            pltpu.VMEM((tok, q.shape[1]), bf16),
            pltpu.VMEM(out_weight.shape, bf16),
            pltpu.SemaphoreType.DMA,
        ],
        cost_estimate=pl.CostEstimate(
            flops=8 * work, transcendentals=work // HEAD_SIZE, bytes_accessed=4 << 20
        ),
        compiler_params=pltpu.CompilerParams(vmem_limit_bytes=52 << 20),
        name="attend",
    )(mine, q, qpos, kpos, *kvs, out_weight)


def expert_rows(pieces, own, other):
    hid, depth = own[0].shape
    width = own[2].shape[1]
    chunks = 4
    deep, wide = depth // chunks, width // chunks
    sizes = [p.shape[0] for p in pieces]
    rows = sum(sizes)
    count = len(pieces)
    starts = [sum(sizes[:i]) for i in range(count)]

    def kernel(*refs):
        ins, refs = refs[:count], refs[count:]
        (ga, ua, da, gb, ub, db), refs = refs[:6], refs[6:]
        outs, refs = refs[:count], refs[count:]
        x, sums, hidden, out, in_sems, out_sems = refs
        fetches = [
            pltpu.make_async_copy(ref, x.at[pl.ds(start, size), :], in_sems.at[i])
            for i, (ref, start, size) in enumerate(zip(ins, starts, sizes))
        ]
        for copy in fetches:
            copy.start()
        for copy in fetches:
            copy.wait()
        sums[...] = jnp.zeros_like(sums)

        @pl.loop(0, chunks)
        def _(k):
            at = pl.ds(pl.multiple_of(k * deep, deep), deep)
            for i, w in enumerate((ga, ua, gb, ub)):
                sums[i] += lax.dot_general(
                    x[:, at], w[:, at], (((1,), (1,)), ((), ())), preferred_element_type=f32
                )

        for i in range(2):
            hidden[i] = (jax.nn.silu(sums[2 * i]) * sums[2 * i + 1]).astype(bf16)

        def out_copies(n):
            at = pl.ds(pl.multiple_of(n * wide, wide), wide)
            for i, ref in enumerate(outs):
                yield pltpu.make_async_copy(
                    out.at[n, pl.ds(starts[i], sizes[i]), :], ref.at[:, at], out_sems.at[n, i]
                )

        @pl.loop(0, chunks)
        def _(n):
            at = pl.ds(pl.multiple_of(n * wide, wide), wide)
            product = jnp.dot(hidden[0], da[:, at], preferred_element_type=f32)
            out[n] = (product + jnp.dot(hidden[1], db[:, at], preferred_element_type=f32)).astype(bf16)
            for copy in out_copies(n):
                copy.start()

        for n in range(chunks):
            for copy in out_copies(n):
                copy.wait()

    far_away = pl.BlockSpec(memory_space=pltpu.HBM)
    return pl.pallas_call(
        kernel,
        out_shape=tuple(jax.ShapeDtypeStruct((size, width), bf16) for size in sizes),
        in_specs=[far_away] * count + [vmem_spec()] * 6,
        out_specs=(far_away,) * count,
        scratch_shapes=[
            pltpu.VMEM((rows, depth), bf16),
            pltpu.VMEM((4, rows, hid), f32),
            pltpu.VMEM((2, rows, hid), bf16),
            pltpu.VMEM((chunks, rows, wide), bf16),
            pltpu.SemaphoreType.DMA((count,)),
            pltpu.SemaphoreType.DMA((chunks, count)),
        ],
        cost_estimate=pl.CostEstimate(
            flops=12 * rows * depth * hid, transcendentals=2 * rows * hid, bytes_accessed=4 * rows * depth
        ),
        compiler_params=pltpu.CompilerParams(vmem_limit_bytes=18 << 20),
        name="expert_rows",
    )(*pieces, *own, *other)


def layer(
    queries,
    keys,
    values,
    resid_in,
    span_order,
    out_weight,
    norm_gain,
    router,
    expert_ids,
    w_gate,
    w_up,
    w_down,
):
    me = lax.axis_index("ctx")
    mine = lax.axis_index("exp").astype(i32)
    my_z, my_x, my_core = me // 8, (me // 2) % RING, me % 2

    kv = jnp.concatenate((keys, values), axis=1)
    near = join(kv, shift(kv, 1, 1), shift(kv, 1, -1), shift(kv, 1, 2))
    left, right = shift(near, 2, 1), shift(near, 2, -1)
    far = shift(near, 2, 2)

    def block_positions(seconds):
        spans = []
        for second in seconds:
            for core in (my_core, 1 - my_core):
                a = jnp.array([0, -1, 1, 2], i32)
                z = jnp.where(core == 0, my_z + second, my_z + a) % RING
                x = jnp.where(core == 0, my_x + a, my_x + second) % RING
                block = z * 8 + x * 2 + core
                spans.append((block[:, None] * 2 + jnp.arange(2, dtype=i32)[None, :]).reshape(-1))
        return positions_of(jnp.concatenate(spans), span_order).reshape(2 * len(seconds), -1)

    query_pos = positions_of(me * 2 + jnp.arange(2, dtype=i32), span_order)
    query_pos = jnp.broadcast_to(query_pos[:, None], (query_pos.shape[0], HEAD_SIZE))
    near_other, far_other = swap(near), swap(far)
    left_other, right_other = swap(left), swap(right)
    sum0, sum1, sum2, sum3 = attend(
        mine.reshape(1),
        queries,
        query_pos,
        block_positions((0, -1, 1, 2)),
        (near, near_other, left, left_other, right, right_other, far, far_other),
        out_weight,
    )

    sub = resid_in.shape[0]
    back2, back1, back3 = shift_exp(sum2, 2), shift_exp(sum1, 1), shift_exp(sum3, 3)
    own_sum = (sum0 + back2.astype(f32)) + (back1.astype(f32) + back3.astype(f32))
    stream = (resid_in.astype(f32) + own_sum).astype(bf16)
    stream_wide = stream.astype(f32)
    mean_square = jnp.mean(stream_wide * stream_wide, axis=-1, keepdims=True)
    normed = (stream_wide * lax.rsqrt(mean_square + 1e-05) * norm_gain).astype(bf16)
    logits = jnp.dot(normed.astype(f32), router, precision=lax.Precision.HIGHEST)
    experts = router.shape[1]
    expert_axis = (mine + jnp.arange(experts, dtype=i32)) % experts
    picked = expert_ids[:, :, None] == jnp.arange(experts, dtype=i32)[None, None, :]
    chosen = jnp.sum(jnp.where(picked, logits[:, None, :], 0.0), axis=-1)
    mixing = jax.nn.softmax(chosen, axis=-1)
    picked = expert_ids[:, :, None] == expert_axis[None, None, :]
    token_weight = jnp.sum(jnp.where(picked, mixing[:, :, None], 0.0), axis=1)
    routed = jnp.any(picked, axis=1)
    rank_of = jnp.cumsum(routed.astype(i32), axis=0) - 1
    slot_count = sub * expert_ids.shape[1] // experts
    slot_axis = jnp.arange(slot_count, dtype=i32)
    placing = jnp.logical_and(routed.T[:, None, :], rank_of.T[:, None, :] == slot_axis[None, :, None])
    outgoing = jnp.dot(
        placing.reshape(experts * slot_count, sub).astype(bf16), normed, preferred_element_type=f32
    ).astype(bf16)
    o0, o1, o2, o3 = (outgoing[i * slot_count : (i + 1) * slot_count] for i in range(4))
    rows = join(o0, shift_exp(o1, 1), shift_exp(o2, 2), shift_exp(o3, 3))

    own = (w_gate[0].T, w_up[0].T, w_down[0])
    other = tuple(swap(w) for w in own)
    n0 = join(rows, shift(rows, 1, 1))
    n1 = join(shift(rows, 1, -1), shift(rows, 1, 2))
    l0, r0 = shift(n0, 2, 1), shift(n0, 2, -1)
    r1, l1 = shift(n1, 2, -1), shift(n1, 2, 1)
    f0, f1 = shift(l0, 2, 1), shift(r1, 2, -1)

    n0, n1 = expert_rows((n0, n1), own, other)
    l0, r1 = expert_rows((l0, r1), own, other)
    l1, r0 = expert_rows((l1, r0), own, other)
    f0, f1 = expert_rows((f0, f1), own, other)

    u0, v1 = shift(l0, 2, -1), shift(r1, 2, 1)
    u1, v0 = shift(l1, 2, -1), shift(r0, 2, 1)
    f0, f1 = shift(f0, 2, 2), shift(f1, 2, 2)
    n0, n1 = total(n0, u0, v0, f0), total(n1, u1, v1, f1)
    part = rows.shape[0]
    back = (shift(n0[part:], 1, -1), shift(n1[:part], 1, 1), shift(n1[part:], 1, 2))
    own_rows = total(n0[:part], *back)

    r0, r1, r2, r3 = (own_rows[i * slot_count : (i + 1) * slot_count] for i in range(4))
    returned = join(r0, shift_exp(r1, 3), shift_exp(r2, 2), shift_exp(r3, 1))
    coefficient = placing.astype(f32) * token_weight.T[:, None, :]
    combined = jnp.einsum("est,esd->td", coefficient, returned.reshape(experts, slot_count, -1).astype(f32))
    return (stream_wide + combined).astype(bf16)


def solution(mesh):
    placed = (
        P("ctx", "exp"),
        P("ctx", "exp"),
        P("ctx", "exp"),
        P(("ctx", "exp"), None),
        P(),
        P("exp", None),
        P(),
        P(),
        P(("ctx", "exp"), None),
        P("exp", None, "ctx"),
        P("exp", None, "ctx"),
        P("exp", "ctx", None),
    )
    return jax.shard_map(layer, mesh=mesh, in_specs=placed, out_specs=P(("ctx", "exp"), None), check_vma=False)
```

```python
import math

import jax
import jax.numpy as jnp
from jax import lax
from jax.experimental import pallas as pl
from jax.experimental.pallas import tpu as pltpu
from jax.sharding import PartitionSpec as P

HEAD_SIZE = 128
SPAN = 64
RING = 4
NEVER = -1e30

f32 = jnp.float32
bf16 = jnp.bfloat16
i32 = jnp.int32


def ctx_index_of(z, x, core):
    return (z % RING) * 8 + (x % RING) * 2 + core


def ring_pairs(phase, step):
    pairs = []
    for z in range(RING):
        for x in range(RING):
            for core in range(2):
                along_x = (core == 0) == (phase == 1)
                target = ctx_index_of(z, x + step, core) if along_x else ctx_index_of(z + step, x, core)
                pairs.append((ctx_index_of(z, x, core), target))
    return pairs


RINGS = {(phase, step): ring_pairs(phase, step) for phase in (1, 2) for step in (1, -1, 2)}
SWAP = [(i, i ^ 1) for i in range(32)]


def shift(a, phase, step):
    return lax.ppermute(a, "ctx", RINGS[phase, step])


def swap(a):
    return lax.ppermute(a, "ctx", SWAP)


def shift_exp(a, step):
    return lax.ppermute(a, "exp", [(i, (i + step) % 4) for i in range(4)])


def join(*parts):
    return jnp.concatenate(parts, axis=0)


def total(*terms):
    return sum(t.astype(f32) for t in terms).astype(bf16)


def positions_of(span_ids, span_order):
    matches = span_ids[:, None] == jnp.arange(span_order.shape[0], dtype=i32)[None, :]
    starts = jnp.sum(jnp.where(matches, span_order[None, :], 0), axis=1) * SPAN
    return (starts[:, None] + jnp.arange(SPAN, dtype=i32)[None, :]).reshape(-1)


def vmem_spec():
    return pl.BlockSpec(memory_space=pltpu.VMEM)


def attend(mine, q, qpos, kpos, kvs, out_weight):
    tok = q.shape[0]
    heads = q.shape[1] // HEAD_SIZE
    kv_heads = kvs[0].shape[1] // (2 * HEAD_SIZE)
    cluster = heads // kv_heads
    rows = cluster * tok
    sub = tok // 4
    width = out_weight.shape[1]
    count = len(kvs)
    slope = math.log2(math.e) / math.sqrt(HEAD_SIZE)

    def kernel(mine_ref, q_ref, qpos_ref, kpos_ref, *refs):
        kv_refs, weight_hbm = refs[:count], refs[count]
        outs = refs[count + 1 : count + 5]
        attended, ordered, weight, sem = refs[count + 5 :]
        fetch = pltpu.make_async_copy(weight_hbm, weight, sem)
        fetch.start()

        @pl.loop(0, kv_heads)
        def _(h):
            def column(i):
                return pl.ds(pl.multiple_of(i * HEAD_SIZE, HEAD_SIZE), HEAD_SIZE)

            q_rows = jnp.concatenate([q_ref[:, column(h * cluster + g)] for g in range(cluster)], axis=0)
            for n, kv in enumerate(kv_refs):
                k = kv[:, column(h)]
                v = kv[:, column(kv_heads + h)]
                s = lax.dot_general(q_rows, k, (((1,), (1,)), ((), ())), preferred_element_type=f32)
                mask = jnp.where(kpos_ref[n : n + 1, :] <= qpos_ref[:, 0:1], 0.0, NEVER)
                s = (s.reshape(cluster, tok, -1) * slope + mask[None]).reshape(rows, -1)
                top = jnp.max(s, axis=1, keepdims=True)
                if n == 0:
                    m = top
                    p = jnp.exp2(s - m)
                    l = jnp.sum(p, axis=1, keepdims=True)
                    acc = jnp.dot(p.astype(bf16), v, preferred_element_type=f32)
                else:
                    new = jnp.maximum(m, top)
                    fade = jnp.exp2(m - new)
                    p = jnp.exp2(s - new)
                    l = l * fade + jnp.sum(p, axis=1, keepdims=True)
                    acc = acc * fade + jnp.dot(p.astype(bf16), v, preferred_element_type=f32)
                    m = new
            result = (acc / l).astype(bf16)
            for g in range(cluster):
                attended[:, column(h * cluster + g)] = result[g * tok : (g + 1) * tok]

        for r in range(4):
            start = pl.multiple_of(lax.rem(mine_ref[0] + r, 4) * sub, sub)
            ordered[r * sub : (r + 1) * sub, :] = attended[pl.ds(start, sub), :]
        fetch.wait()

        @pl.loop(0, 4)
        def _(n):
            at = pl.ds(pl.multiple_of(n * (width // 4), width // 4), width // 4)
            product = jnp.dot(ordered[...], weight[:, at], preferred_element_type=f32)
            for r in range(4):
                outs[r][:, at] = product[r * sub : (r + 1) * sub].astype(outs[r].dtype)

    work = q.shape[0] * q.shape[1] * sum(kv.shape[0] for kv in kvs)
    return pl.pallas_call(
        kernel,
        out_shape=tuple(jax.ShapeDtypeStruct((sub, width), t) for t in (f32, bf16, bf16, bf16)),
        in_specs=[pl.BlockSpec(memory_space=pltpu.SMEM)] + [vmem_spec()] * (count + 3)
        + [pl.BlockSpec(memory_space=pltpu.HBM)],
        out_specs=(vmem_spec(),) * 4,
        scratch_shapes=[
            pltpu.VMEM((tok, q.shape[1]), bf16),
            pltpu.VMEM((tok, q.shape[1]), bf16),
            pltpu.VMEM(out_weight.shape, bf16),
            pltpu.SemaphoreType.DMA,
        ],
        cost_estimate=pl.CostEstimate(
            flops=8 * work, transcendentals=work // HEAD_SIZE, bytes_accessed=4 << 20
        ),
        compiler_params=pltpu.CompilerParams(vmem_limit_bytes=52 << 20),
        name="attend",
    )(mine, q, qpos, kpos, *kvs, out_weight)


def expert_rows(pieces, own, other):
    hid, depth = own[0].shape
    width = own[2].shape[1]
    chunks = 4
    deep, wide = depth // chunks, width // chunks
    sizes = [p.shape[0] for p in pieces]
    rows = sum(sizes)
    count = len(pieces)
    starts = [sum(sizes[:i]) for i in range(count)]

    def kernel(*refs):
        ins, refs = refs[:count], refs[count:]
        (ga, ua, da, gb, ub, db), refs = refs[:6], refs[6:]
        outs, refs = refs[:count], refs[count:]
        x, w, dw, sums, hidden, out, x_sems, w_sems, d_sems, out_sems = refs

        def first_copies(k):
            at = pl.ds(pl.multiple_of(k * deep, deep), deep)
            for i, ref in enumerate((ga, gb, ua, ub)):
                yield pltpu.make_async_copy(ref.at[:, at], w.at[k, pl.ds(i * hid, hid), :], w_sems.at[k, i])
            for i, ref in enumerate(ins):
                yield pltpu.make_async_copy(
                    ref.at[:, at], x.at[k, pl.ds(starts[i], sizes[i]), :], x_sems.at[k, i]
                )

        def last_copies(n):
            at = pl.ds(pl.multiple_of(n * wide, wide), wide)
            for i, ref in enumerate((da, db)):
                yield pltpu.make_async_copy(ref.at[:, at], dw.at[n, pl.ds(i * hid, hid), :], d_sems.at[n, i])

        def out_copies(n):
            at = pl.ds(pl.multiple_of(n * wide, wide), wide)
            for i, ref in enumerate(outs):
                yield pltpu.make_async_copy(
                    out.at[n, pl.ds(starts[i], sizes[i]), :], ref.at[:, at], out_sems.at[n, i]
                )

        for k in range(chunks):
            for copy in first_copies(k):
                copy.start()
        for n in range(chunks):
            for copy in last_copies(n):
                copy.start()
        sums[...] = jnp.zeros_like(sums)

        @pl.loop(0, chunks)
        def _(k):
            for copy in first_copies(k):
                copy.wait()
            sums[...] += lax.dot_general(x[k], w[k], (((1,), (1,)), ((), ())), preferred_element_type=f32)

        hidden[...] = (jax.nn.silu(sums[:, : 2 * hid]) * sums[:, 2 * hid :]).astype(bf16)

        @pl.loop(0, chunks)
        def _(n):
            for copy in last_copies(n):
                copy.wait()
            out[n] = jnp.dot(hidden[...], dw[n], preferred_element_type=f32).astype(bf16)
            for copy in out_copies(n):
                copy.start()

        for n in range(chunks):
            for copy in out_copies(n):
                copy.wait()

    anywhere = pl.BlockSpec(memory_space=pltpu.HBM)
    return pl.pallas_call(
        kernel,
        out_shape=tuple(jax.ShapeDtypeStruct((size, width), bf16) for size in sizes),
        in_specs=[anywhere] * (count + 6),
        out_specs=(anywhere,) * count,
        scratch_shapes=[
            pltpu.VMEM((chunks, rows, deep), bf16),
            pltpu.VMEM((chunks, 4 * hid, deep), bf16),
            pltpu.VMEM((chunks, 2 * hid, wide), bf16),
            pltpu.VMEM((rows, 4 * hid), f32),
            pltpu.VMEM((rows, 2 * hid), bf16),
            pltpu.VMEM((chunks, rows, wide), bf16),
            pltpu.SemaphoreType.DMA((chunks, count)),
            pltpu.SemaphoreType.DMA((chunks, 4)),
            pltpu.SemaphoreType.DMA((chunks, 2)),
            pltpu.SemaphoreType.DMA((chunks, count)),
        ],
        cost_estimate=pl.CostEstimate(
            flops=12 * rows * depth * hid, transcendentals=2 * rows * hid, bytes_accessed=12 * depth * hid
        ),
        compiler_params=pltpu.CompilerParams(vmem_limit_bytes=(26 << 20) + rows * (32 << 10)),
        name="expert_rows",
    )(*pieces, *own, *other)


def layer(
    queries,
    keys,
    values,
    resid_in,
    span_order,
    out_weight,
    norm_gain,
    router,
    expert_ids,
    w_gate,
    w_up,
    w_down,
):
    me = lax.axis_index("ctx")
    mine = lax.axis_index("exp").astype(i32)
    my_z, my_x, my_core = me // 8, (me // 2) % RING, me % 2

    kv = jnp.concatenate((keys, values), axis=1)
    near = join(kv, shift(kv, 1, 1), shift(kv, 1, -1), shift(kv, 1, 2))
    left, right = shift(near, 2, 1), shift(near, 2, -1)
    far = shift(near, 2, 2)

    def block_positions(seconds):
        spans = []
        for second in seconds:
            for core in (my_core, 1 - my_core):
                a = jnp.array([0, -1, 1, 2], i32)
                z = jnp.where(core == 0, my_z + second, my_z + a) % RING
                x = jnp.where(core == 0, my_x + a, my_x + second) % RING
                block = z * 8 + x * 2 + core
                spans.append((block[:, None] * 2 + jnp.arange(2, dtype=i32)[None, :]).reshape(-1))
        return positions_of(jnp.concatenate(spans), span_order).reshape(2 * len(seconds), -1)

    query_pos = positions_of(me * 2 + jnp.arange(2, dtype=i32), span_order)
    query_pos = jnp.broadcast_to(query_pos[:, None], (query_pos.shape[0], HEAD_SIZE))
    near_other, far_other = swap(near), swap(far)
    left_other, right_other = swap(left), swap(right)
    sum0, sum1, sum2, sum3 = attend(
        mine.reshape(1),
        queries,
        query_pos,
        block_positions((0, -1, 1, 2)),
        (near, near_other, left, left_other, right, right_other, far, far_other),
        out_weight,
    )

    sub = resid_in.shape[0]
    back2, back1, back3 = shift_exp(sum2, 2), shift_exp(sum1, 1), shift_exp(sum3, 3)
    own_sum = (sum0 + back2.astype(f32)) + (back1.astype(f32) + back3.astype(f32))
    stream = (resid_in.astype(f32) + own_sum).astype(bf16)
    stream_wide = stream.astype(f32)
    mean_square = jnp.mean(stream_wide * stream_wide, axis=-1, keepdims=True)
    normed = (stream_wide * lax.rsqrt(mean_square + 1e-05) * norm_gain).astype(bf16)
    logits = jnp.dot(normed.astype(f32), router, precision=lax.Precision.HIGHEST)
    experts = router.shape[1]
    expert_axis = (mine + jnp.arange(experts, dtype=i32)) % experts
    picked = expert_ids[:, :, None] == jnp.arange(experts, dtype=i32)[None, None, :]
    chosen = jnp.sum(jnp.where(picked, logits[:, None, :], 0.0), axis=-1)
    mixing = jax.nn.softmax(chosen, axis=-1)
    picked = expert_ids[:, :, None] == expert_axis[None, None, :]
    token_weight = jnp.sum(jnp.where(picked, mixing[:, :, None], 0.0), axis=1)
    routed = jnp.any(picked, axis=1)
    rank_of = jnp.cumsum(routed.astype(i32), axis=0) - 1
    slot_count = sub * expert_ids.shape[1] // experts
    slot_axis = jnp.arange(slot_count, dtype=i32)
    placing = jnp.logical_and(routed.T[:, None, :], rank_of.T[:, None, :] == slot_axis[None, :, None])
    outgoing = jnp.dot(
        placing.reshape(experts * slot_count, sub).astype(bf16), normed, preferred_element_type=f32
    ).astype(bf16)
    o0, o1, o2, o3 = (outgoing[i * slot_count : (i + 1) * slot_count] for i in range(4))
    rows = join(o0, shift_exp(o1, 1), shift_exp(o2, 2), shift_exp(o3, 3))

    own = (w_gate[0].T, w_up[0].T, w_down[0])
    other = tuple(swap(w) for w in own)
    n0 = join(rows, shift(rows, 1, 1))
    n1 = join(shift(rows, 1, -1), shift(rows, 1, 2))
    l0, r0 = shift(n0, 2, 1), shift(n0, 2, -1)
    r1, l1 = shift(n1, 2, -1), shift(n1, 2, 1)
    f0, f1 = shift(l0, 2, 1), shift(r1, 2, -1)

    n0, n1 = expert_rows((n0, n1), own, other)
    l0, r1 = expert_rows((l0, r1), own, other)
    l1, r0 = expert_rows((l1, r0), own, other)
    f0, f1 = expert_rows((f0, f1), own, other)

    u0, v1 = shift(l0, 2, -1), shift(r1, 2, 1)
    u1, v0 = shift(l1, 2, -1), shift(r0, 2, 1)
    f0, f1 = shift(f0, 2, 2), shift(f1, 2, 2)
    n0, n1 = total(n0, u0, v0, f0), total(n1, u1, v1, f1)
    part = rows.shape[0]
    back = (shift(n0[part:], 1, -1), shift(n1[:part], 1, 1), shift(n1[part:], 1, 2))
    own_rows = total(n0[:part], *back)

    r0, r1, r2, r3 = (own_rows[i * slot_count : (i + 1) * slot_count] for i in range(4))
    returned = join(r0, shift_exp(r1, 3), shift_exp(r2, 2), shift_exp(r3, 1))
    coefficient = placing.astype(f32) * token_weight.T[:, None, :]
    combined = jnp.einsum("est,esd->td", coefficient, returned.reshape(experts, slot_count, -1).astype(f32))
    return (stream_wide + combined).astype(bf16)


def solution(mesh):
    placed = (
        P("ctx", "exp"),
        P("ctx", "exp"),
        P("ctx", "exp"),
        P(("ctx", "exp"), None),
        P(),
        P("exp", None),
        P(),
        P(),
        P(("ctx", "exp"), None),
        P("exp", None, "ctx"),
        P("exp", None, "ctx"),
        P("exp", "ctx", None),
    )
    return jax.shard_map(layer, mesh=mesh, in_specs=placed, out_specs=P(("ctx", "exp"), None), check_vma=False)
```

```python
import math

import jax
import jax.numpy as jnp
from jax import lax
from jax.experimental import pallas as pl
from jax.experimental.pallas import tpu as pltpu
from jax.sharding import PartitionSpec as P

HEAD_SIZE = 128
SPAN = 64
RING = 4
NEVER = -1e30

f32 = jnp.float32
bf16 = jnp.bfloat16
i32 = jnp.int32


def ctx_index_of(z, x, core):
    return (z % RING) * 8 + (x % RING) * 2 + core


def ring_pairs(phase, step):
    pairs = []
    for z in range(RING):
        for x in range(RING):
            for core in range(2):
                along_x = (core == 0) == (phase == 1)
                target = ctx_index_of(z, x + step, core) if along_x else ctx_index_of(z + step, x, core)
                pairs.append((ctx_index_of(z, x, core), target))
    return pairs


RINGS = {(phase, step): ring_pairs(phase, step) for phase in (1, 2) for step in (1, -1, 2)}
SWAP = [(i, i ^ 1) for i in range(32)]


def shift(a, phase, step):
    return lax.ppermute(a, "ctx", RINGS[phase, step])


def swap(a):
    return lax.ppermute(a, "ctx", SWAP)


def shift_exp(a, step):
    return lax.ppermute(a, "exp", [(i, (i + step) % 4) for i in range(4)])


def join(*parts):
    return jnp.concatenate(parts, axis=0)


def total(*terms):
    return sum(t.astype(f32) for t in terms).astype(bf16)


def positions_of(span_ids, span_order):
    matches = span_ids[:, None] == jnp.arange(span_order.shape[0], dtype=i32)[None, :]
    starts = jnp.sum(jnp.where(matches, span_order[None, :], 0), axis=1) * SPAN
    return (starts[:, None] + jnp.arange(SPAN, dtype=i32)[None, :]).reshape(-1)


def vmem_spec():
    return pl.BlockSpec(memory_space=pltpu.VMEM)


def attend(mine, q, qpos, kpos, kvs, out_weight):
    tok = q.shape[0]
    heads = q.shape[1] // HEAD_SIZE
    kv_heads = kvs[0].shape[1] // (2 * HEAD_SIZE)
    cluster = heads // kv_heads
    rows = cluster * tok
    sub = tok // 4
    width = out_weight.shape[1]
    count = len(kvs)
    slope = math.log2(math.e) / math.sqrt(HEAD_SIZE)

    def kernel(mine_ref, q_ref, qpos_ref, kpos_ref, *refs):
        kv_refs, weight_hbm = refs[:count], refs[count]
        outs = refs[count + 1 : count + 5]
        attended, ordered, weight, sem = refs[count + 5 :]
        fetch = pltpu.make_async_copy(weight_hbm, weight, sem)
        fetch.start()

        @pl.loop(0, kv_heads)
        def _(h):
            def column(i):
                return pl.ds(pl.multiple_of(i * HEAD_SIZE, HEAD_SIZE), HEAD_SIZE)

            q_rows = jnp.concatenate([q_ref[:, column(h * cluster + g)] for g in range(cluster)], axis=0)
            for n, kv in enumerate(kv_refs):
                k = kv[:, column(h)]
                v = kv[:, column(kv_heads + h)]
                s = lax.dot_general(q_rows, k, (((1,), (1,)), ((), ())), preferred_element_type=f32)
                mask = jnp.where(kpos_ref[n : n + 1, :] <= qpos_ref[:, 0:1], 0.0, NEVER)
                s = (s.reshape(cluster, tok, -1) * slope + mask[None]).reshape(rows, -1)
                top = jnp.max(s, axis=1, keepdims=True)
                if n == 0:
                    m = top
                    p = jnp.exp2(s - m)
                    l = jnp.sum(p, axis=1, keepdims=True)
                    acc = jnp.dot(p.astype(bf16), v, preferred_element_type=f32)
                else:
                    new = jnp.maximum(m, top)
                    fade = jnp.exp2(m - new)
                    p = jnp.exp2(s - new)
                    l = l * fade + jnp.sum(p, axis=1, keepdims=True)
                    acc = acc * fade + jnp.dot(p.astype(bf16), v, preferred_element_type=f32)
                    m = new
            result = (acc / l).astype(bf16)
            for g in range(cluster):
                attended[:, column(h * cluster + g)] = result[g * tok : (g + 1) * tok]

        for r in range(4):
            start = pl.multiple_of(lax.rem(mine_ref[0] + r, 4) * sub, sub)
            ordered[r * sub : (r + 1) * sub, :] = attended[pl.ds(start, sub), :]
        fetch.wait()

        @pl.loop(0, 4)
        def _(n):
            at = pl.ds(pl.multiple_of(n * (width // 4), width // 4), width // 4)
            product = jnp.dot(ordered[...], weight[:, at], preferred_element_type=f32)
            for r in range(4):
                outs[r][:, at] = product[r * sub : (r + 1) * sub].astype(outs[r].dtype)

    work = q.shape[0] * q.shape[1] * sum(kv.shape[0] for kv in kvs)
    return pl.pallas_call(
        kernel,
        out_shape=tuple(jax.ShapeDtypeStruct((sub, width), t) for t in (f32, bf16, bf16, bf16)),
        in_specs=[pl.BlockSpec(memory_space=pltpu.SMEM)] + [vmem_spec()] * (count + 3)
        + [pl.BlockSpec(memory_space=pltpu.HBM)],
        out_specs=(vmem_spec(),) * 4,
        scratch_shapes=[
            pltpu.VMEM((tok, q.shape[1]), bf16),
            pltpu.VMEM((tok, q.shape[1]), bf16),
            pltpu.VMEM(out_weight.shape, bf16),
            pltpu.SemaphoreType.DMA,
        ],
        cost_estimate=pl.CostEstimate(
            flops=8 * work, transcendentals=work // HEAD_SIZE, bytes_accessed=4 << 20
        ),
        compiler_params=pltpu.CompilerParams(vmem_limit_bytes=52 << 20),
        name="attend",
    )(mine, q, qpos, kpos, *kvs, out_weight)


def expert_rows(pieces, own, other):
    hid, depth = own[0].shape
    width = own[2].shape[1]
    chunks, panels = 4, 4
    deep, wide = depth // chunks, width // panels
    sizes = [p.shape[0] for p in pieces]
    rows = sum(sizes)
    count = len(pieces)
    starts = [sum(sizes[:i]) for i in range(count)]

    def kernel(*refs):
        ins, refs = refs[:count], refs[count:]
        (ga, ua, da, gb, ub, db), refs = refs[:6], refs[6:]
        outs, refs = refs[:count], refs[count:]
        x, w, dw, sums, hidden, out, x_sems, w_sems, d_sems, out_sems = refs

        def first_copies(k):
            at = pl.ds(pl.multiple_of(k * deep, deep), deep)
            for i, ref in enumerate((ga, gb, ua, ub)):
                yield pltpu.make_async_copy(ref.at[:, at], w.at[k, pl.ds(i * hid, hid), :], w_sems.at[k, i])
            for i, ref in enumerate(ins):
                yield pltpu.make_async_copy(
                    ref.at[:, at], x.at[k, pl.ds(starts[i], sizes[i]), :], x_sems.at[k, i]
                )

        def last_copies(n):
            at = pl.ds(pl.multiple_of(n * wide, wide), wide)
            for i, ref in enumerate((da, db)):
                yield pltpu.make_async_copy(ref.at[:, at], dw.at[n, pl.ds(i * hid, hid), :], d_sems.at[n, i])

        def out_copies(n):
            at = pl.ds(pl.multiple_of(n * wide, wide), wide)
            for i, ref in enumerate(outs):
                yield pltpu.make_async_copy(
                    out.at[n, pl.ds(starts[i], sizes[i]), :], ref.at[:, at], out_sems.at[n, i]
                )

        for k in range(chunks):
            for copy in first_copies(k):
                copy.start()
        for n in range(panels):
            for copy in last_copies(n):
                copy.start()
        sums[...] = jnp.zeros_like(sums)

        @pl.loop(0, chunks)
        def _(k):
            for copy in first_copies(k):
                copy.wait()
            sums[...] += lax.dot_general(x[k], w[k], (((1,), (1,)), ((), ())), preferred_element_type=f32)

        hidden[...] = (jax.nn.silu(sums[:, : 2 * hid]) * sums[:, 2 * hid :]).astype(bf16)

        @pl.loop(0, panels)
        def _(n):
            for copy in last_copies(n):
                copy.wait()
            out[n] = jnp.dot(hidden[...], dw[n], preferred_element_type=f32).astype(bf16)
            for copy in out_copies(n):
                copy.start()

        for n in range(panels):
            for copy in out_copies(n):
                copy.wait()

    anywhere = pl.BlockSpec(memory_space=pltpu.HBM)
    return pl.pallas_call(
        kernel,
        out_shape=tuple(jax.ShapeDtypeStruct((size, width), bf16) for size in sizes),
        in_specs=[anywhere] * (count + 6),
        out_specs=(anywhere,) * count,
        scratch_shapes=[
            pltpu.VMEM((chunks, rows, deep), bf16),
            pltpu.VMEM((chunks, 4 * hid, deep), bf16),
            pltpu.VMEM((panels, 2 * hid, wide), bf16),
            pltpu.VMEM((rows, 4 * hid), f32),
            pltpu.VMEM((rows, 2 * hid), bf16),
            pltpu.VMEM((panels, rows, wide), bf16),
            pltpu.SemaphoreType.DMA((chunks, count)),
            pltpu.SemaphoreType.DMA((chunks, 4)),
            pltpu.SemaphoreType.DMA((panels, 2)),
            pltpu.SemaphoreType.DMA((panels, count)),
        ],
        cost_estimate=pl.CostEstimate(
            flops=12 * rows * depth * hid, transcendentals=2 * rows * hid, bytes_accessed=12 * depth * hid
        ),
        compiler_params=pltpu.CompilerParams(vmem_limit_bytes=(26 << 20) + rows * (32 << 10)),
        name="expert_rows",
    )(*pieces, *own, *other)


def layer(
    queries,
    keys,
    values,
    resid_in,
    span_order,
    out_weight,
    norm_gain,
    router,
    expert_ids,
    w_gate,
    w_up,
    w_down,
):
    me = lax.axis_index("ctx")
    mine = lax.axis_index("exp").astype(i32)
    my_z, my_x, my_core = me // 8, (me // 2) % RING, me % 2

    kv = jnp.concatenate((keys, values), axis=1)
    near = join(kv, shift(kv, 1, 1), shift(kv, 1, -1), shift(kv, 1, 2))
    left, right = shift(near, 2, 1), shift(near, 2, -1)
    far = shift(near, 2, 2)

    def block_positions(seconds):
        spans = []
        for second in seconds:
            for core in (my_core, 1 - my_core):
                a = jnp.array([0, -1, 1, 2], i32)
                z = jnp.where(core == 0, my_z + second, my_z + a) % RING
                x = jnp.where(core == 0, my_x + a, my_x + second) % RING
                block = z * 8 + x * 2 + core
                spans.append((block[:, None] * 2 + jnp.arange(2, dtype=i32)[None, :]).reshape(-1))
        return positions_of(jnp.concatenate(spans), span_order).reshape(2 * len(seconds), -1)

    query_pos = positions_of(me * 2 + jnp.arange(2, dtype=i32), span_order)
    query_pos = jnp.broadcast_to(query_pos[:, None], (query_pos.shape[0], HEAD_SIZE))
    near_other, far_other = swap(near), swap(far)
    left_other, right_other = swap(left), swap(right)
    sum0, sum1, sum2, sum3 = attend(
        mine.reshape(1),
        queries,
        query_pos,
        block_positions((0, -1, 1, 2)),
        (near, near_other, left, left_other, right, right_other, far, far_other),
        out_weight,
    )

    sub = resid_in.shape[0]
    back2, back1, back3 = shift_exp(sum2, 2), shift_exp(sum1, 1), shift_exp(sum3, 3)
    own_sum = (sum0 + back2.astype(f32)) + (back1.astype(f32) + back3.astype(f32))
    stream = (resid_in.astype(f32) + own_sum).astype(bf16)
    stream_wide = stream.astype(f32)
    mean_square = jnp.mean(stream_wide * stream_wide, axis=-1, keepdims=True)
    normed = (stream_wide * lax.rsqrt(mean_square + 1e-05) * norm_gain).astype(bf16)
    logits = jnp.dot(normed.astype(f32), router, precision=lax.Precision.HIGHEST)
    experts = router.shape[1]
    expert_axis = (mine + jnp.arange(experts, dtype=i32)) % experts
    picked = expert_ids[:, :, None] == jnp.arange(experts, dtype=i32)[None, None, :]
    chosen = jnp.sum(jnp.where(picked, logits[:, None, :], 0.0), axis=-1)
    mixing = jax.nn.softmax(chosen, axis=-1)
    picked = expert_ids[:, :, None] == expert_axis[None, None, :]
    token_weight = jnp.sum(jnp.where(picked, mixing[:, :, None], 0.0), axis=1)
    routed = jnp.any(picked, axis=1)
    rank_of = jnp.cumsum(routed.astype(i32), axis=0) - 1
    slot_count = sub * expert_ids.shape[1] // experts
    slot_axis = jnp.arange(slot_count, dtype=i32)
    placing = jnp.logical_and(routed.T[:, None, :], rank_of.T[:, None, :] == slot_axis[None, :, None])
    outgoing = jnp.dot(
        placing.reshape(experts * slot_count, sub).astype(bf16), normed, preferred_element_type=f32
    ).astype(bf16)
    o0, o1, o2, o3 = (outgoing[i * slot_count : (i + 1) * slot_count] for i in range(4))
    rows = join(o0, shift_exp(o1, 1), shift_exp(o2, 2), shift_exp(o3, 3))

    own = (w_gate[0].T, w_up[0].T, w_down[0])
    other = tuple(swap(w) for w in own)
    half = rows.shape[0] // 2
    beside0, beside1 = shift(rows, 1, 1), shift(rows, 1, -1)
    n0 = join(rows, beside0)
    n1 = join(beside1, shift(beside0[:half], 1, 1), shift(beside1[half:], 1, -1))
    l0, r0 = shift(n0, 2, 1), shift(n0, 2, -1)
    r1, l1 = shift(n1, 2, -1), shift(n1, 2, 1)
    f0, f1 = shift(l0, 2, 1), shift(r1, 2, -1)

    n0, n1 = expert_rows((n0, n1), own, other)
    l0, r1 = expert_rows((l0, r1), own, other)
    l1, r0 = expert_rows((l1, r0), own, other)
    f0, f1 = expert_rows((f0, f1), own, other)

    u1, v0 = shift(l1, 2, -1), shift(r0, 2, 1)
    q0, q1 = shift(f0, 2, -1), shift(f1, 2, 1)
    u0, v1 = shift(total(l0, q0), 2, -1), shift(total(r1, q1), 2, 1)
    level = lax.ppermute(v1[:16, :128], "ctx", [(2 * i, 2 * i + 1) for i in range(16)])
    n0, n1 = total(n0, u0, v0), total(n1, u1, v1)
    part = rows.shape[0]
    back = (shift(n0[part:], 1, -1), shift(n1[:part], 1, 1), shift(n1[part:], 1, 2))
    own_rows = total(n0[:part] + jnp.max(level) * 0, *back)

    r0, r1, r2, r3 = (own_rows[i * slot_count : (i + 1) * slot_count] for i in range(4))
    returned = join(r0, shift_exp(r1, 3), shift_exp(r2, 2), shift_exp(r3, 1))
    coefficient = placing.astype(f32) * token_weight.T[:, None, :]
    combined = jnp.einsum("est,esd->td", coefficient, returned.reshape(experts, slot_count, -1).astype(f32))
    return (stream_wide + combined).astype(bf16)


def solution(mesh):
    placed = (
        P("ctx", "exp"),
        P("ctx", "exp"),
        P("ctx", "exp"),
        P(("ctx", "exp"), None),
        P(),
        P("exp", None),
        P(),
        P(),
        P(("ctx", "exp"), None),
        P("exp", None, "ctx"),
        P("exp", None, "ctx"),
        P("exp", "ctx", None),
    )
    return jax.shard_map(layer, mesh=mesh, in_specs=placed, out_specs=P(("ctx", "exp"), None), check_vma=False)
```

```python
import math

import jax
import jax.numpy as jnp
from jax import lax
from jax.experimental import pallas as pl
from jax.experimental.pallas import tpu as pltpu
from jax.sharding import PartitionSpec as P

HEAD_SIZE = 128
SPAN = 64
RING = 4
NEVER = -1e30

f32 = jnp.float32
bf16 = jnp.bfloat16
i32 = jnp.int32


def ctx_index_of(z, x, core):
    return (z % RING) * 8 + (x % RING) * 2 + core


def ring_pairs(phase, step):
    pairs = []
    for z in range(RING):
        for x in range(RING):
            for core in range(2):
                along_x = (core == 0) == (phase == 1)
                target = ctx_index_of(z, x + step, core) if along_x else ctx_index_of(z + step, x, core)
                pairs.append((ctx_index_of(z, x, core), target))
    return pairs


RINGS = {(phase, step): ring_pairs(phase, step) for phase in (1, 2) for step in (1, -1, 2)}
SWAP = [(i, i ^ 1) for i in range(32)]


def shift(a, phase, step):
    return lax.ppermute(a, "ctx", RINGS[phase, step])


def swap(a):
    return lax.ppermute(a, "ctx", SWAP)


def shift_exp(a, step):
    return lax.ppermute(a, "exp", [(i, (i + step) % 4) for i in range(4)])


def join(*parts):
    return jnp.concatenate(parts, axis=0)


def total(*terms):
    return sum(t.astype(f32) for t in terms).astype(bf16)


def positions_of(span_ids, span_order):
    matches = span_ids[:, None] == jnp.arange(span_order.shape[0], dtype=i32)[None, :]
    starts = jnp.sum(jnp.where(matches, span_order[None, :], 0), axis=1) * SPAN
    return (starts[:, None] + jnp.arange(SPAN, dtype=i32)[None, :]).reshape(-1)


def vmem_spec():
    return pl.BlockSpec(memory_space=pltpu.VMEM)


def attend(mine, q, qpos, kpos, kvs, out_weight):
    tok = q.shape[0]
    heads = q.shape[1] // HEAD_SIZE
    kv_heads = kvs[0].shape[1] // (2 * HEAD_SIZE)
    cluster = heads // kv_heads
    rows = cluster * tok
    sub = tok // 4
    width = out_weight.shape[1]
    count = len(kvs)
    slope = math.log2(math.e) / math.sqrt(HEAD_SIZE)

    def kernel(mine_ref, q_ref, qpos_ref, kpos_ref, *refs):
        kv_refs, weight_hbm = refs[:count], refs[count]
        outs = refs[count + 1 : count + 5]
        attended, ordered, weight, sem = refs[count + 5 :]
        fetch = pltpu.make_async_copy(weight_hbm, weight, sem)
        fetch.start()

        @pl.loop(0, kv_heads)
        def _(h):
            def column(i):
                return pl.ds(pl.multiple_of(i * HEAD_SIZE, HEAD_SIZE), HEAD_SIZE)

            q_rows = jnp.concatenate([q_ref[:, column(h * cluster + g)] for g in range(cluster)], axis=0)

            def score(kv):
                contract = (((1,), (1,)), ((), ()))
                return lax.dot_general(q_rows, kv[:, column(h)], contract, preferred_element_type=f32)

            ahead = score(kv_refs[0])
            for n, kv in enumerate(kv_refs):
                s = ahead
                if n + 1 < count:
                    ahead = score(kv_refs[n + 1])
                v = kv[:, column(kv_heads + h)]
                mask = jnp.where(kpos_ref[n : n + 1, :] <= qpos_ref[:, 0:1], 0.0, NEVER)
                s = (s.reshape(cluster, tok, -1) * slope + mask[None]).reshape(rows, -1)
                top = jnp.max(s, axis=1, keepdims=True)
                if n == 0:
                    m = top
                    p = jnp.exp2(s - m)
                    l = jnp.sum(p, axis=1, keepdims=True)
                    acc = jnp.dot(p.astype(bf16), v, preferred_element_type=f32)
                else:
                    new = jnp.maximum(m, top)
                    fade = jnp.exp2(m - new)
                    p = jnp.exp2(s - new)
                    l = l * fade + jnp.sum(p, axis=1, keepdims=True)
                    acc = acc * fade + jnp.dot(p.astype(bf16), v, preferred_element_type=f32)
                    m = new
            result = (acc / l).astype(bf16)
            for g in range(cluster):
                attended[:, column(h * cluster + g)] = result[g * tok : (g + 1) * tok]

        for r in range(4):
            start = pl.multiple_of(lax.rem(mine_ref[0] + r, 4) * sub, sub)
            ordered[r * sub : (r + 1) * sub, :] = attended[pl.ds(start, sub), :]
        fetch.wait()

        @pl.loop(0, 4)
        def _(n):
            at = pl.ds(pl.multiple_of(n * (width // 4), width // 4), width // 4)
            product = jnp.dot(ordered[...], weight[:, at], preferred_element_type=f32)
            for r in range(4):
                outs[r][:, at] = product[r * sub : (r + 1) * sub].astype(outs[r].dtype)

    work = q.shape[0] * q.shape[1] * sum(kv.shape[0] for kv in kvs)
    return pl.pallas_call(
        kernel,
        out_shape=tuple(jax.ShapeDtypeStruct((sub, width), t) for t in (f32, bf16, bf16, bf16)),
        in_specs=[pl.BlockSpec(memory_space=pltpu.SMEM)] + [vmem_spec()] * (count + 3)
        + [pl.BlockSpec(memory_space=pltpu.HBM)],
        out_specs=(vmem_spec(),) * 4,
        scratch_shapes=[
            pltpu.VMEM((tok, q.shape[1]), bf16),
            pltpu.VMEM((tok, q.shape[1]), bf16),
            pltpu.VMEM(out_weight.shape, bf16),
            pltpu.SemaphoreType.DMA,
        ],
        cost_estimate=pl.CostEstimate(
            flops=8 * work, transcendentals=work // HEAD_SIZE, bytes_accessed=4 << 20
        ),
        compiler_params=pltpu.CompilerParams(vmem_limit_bytes=52 << 20),
        name="attend",
    )(mine, q, qpos, kpos, *kvs, out_weight)


def expert_rows(pieces, own, other):
    hid, depth = own[0].shape
    width = own[2].shape[1]
    chunks, panels = 4, 4
    deep, wide = depth // chunks, width // panels
    sizes = [p.shape[0] for p in pieces]
    rows = sum(sizes)
    count = len(pieces)
    starts = [sum(sizes[:i]) for i in range(count)]

    def kernel(*refs):
        ins, refs = refs[:count], refs[count:]
        (ga, ua, da, gb, ub, db), refs = refs[:6], refs[6:]
        outs, refs = refs[:count], refs[count:]
        x, w, dw, sums, hidden, out, x_sems, w_sems, d_sems, out_sems = refs

        def first_copies(k):
            at = pl.ds(pl.multiple_of(k * deep, deep), deep)
            for i, ref in enumerate((ga, gb, ua, ub)):
                yield pltpu.make_async_copy(ref.at[:, at], w.at[k, pl.ds(i * hid, hid), :], w_sems.at[k, i])
            for i, ref in enumerate(ins):
                yield pltpu.make_async_copy(
                    ref.at[:, at], x.at[k, pl.ds(starts[i], sizes[i]), :], x_sems.at[k, i]
                )

        def last_copies(n):
            at = pl.ds(pl.multiple_of(n * wide, wide), wide)
            for i, ref in enumerate((da, db)):
                yield pltpu.make_async_copy(ref.at[:, at], dw.at[n, pl.ds(i * hid, hid), :], d_sems.at[n, i])

        def out_copies(n):
            at = pl.ds(pl.multiple_of(n * wide, wide), wide)
            for i, ref in enumerate(outs):
                yield pltpu.make_async_copy(
                    out.at[n, pl.ds(starts[i], sizes[i]), :], ref.at[:, at], out_sems.at[n, i]
                )

        for k in range(chunks):
            for copy in first_copies(k):
                copy.start()
        for n in range(panels):
            for copy in last_copies(n):
                copy.start()
        sums[...] = jnp.zeros_like(sums)

        @pl.loop(0, chunks)
        def _(k):
            for copy in first_copies(k):
                copy.wait()
            sums[...] += lax.dot_general(x[k], w[k], (((1,), (1,)), ((), ())), preferred_element_type=f32)

        hidden[...] = (jax.nn.silu(sums[:, : 2 * hid]) * sums[:, 2 * hid :]).astype(bf16)

        @pl.loop(0, panels)
        def _(n):
            for copy in last_copies(n):
                copy.wait()
            out[n] = jnp.dot(hidden[...], dw[n], preferred_element_type=f32).astype(bf16)
            for copy in out_copies(n):
                copy.start()

        for n in range(panels):
            for copy in out_copies(n):
                copy.wait()

    anywhere = pl.BlockSpec(memory_space=pltpu.HBM)
    return pl.pallas_call(
        kernel,
        out_shape=tuple(jax.ShapeDtypeStruct((size, width), bf16) for size in sizes),
        in_specs=[anywhere] * (count + 6),
        out_specs=(anywhere,) * count,
        scratch_shapes=[
            pltpu.VMEM((chunks, rows, deep), bf16),
            pltpu.VMEM((chunks, 4 * hid, deep), bf16),
            pltpu.VMEM((panels, 2 * hid, wide), bf16),
            pltpu.VMEM((rows, 4 * hid), f32),
            pltpu.VMEM((rows, 2 * hid), bf16),
            pltpu.VMEM((panels, rows, wide), bf16),
            pltpu.SemaphoreType.DMA((chunks, count)),
            pltpu.SemaphoreType.DMA((chunks, 4)),
            pltpu.SemaphoreType.DMA((panels, 2)),
            pltpu.SemaphoreType.DMA((panels, count)),
        ],
        cost_estimate=pl.CostEstimate(
            flops=12 * rows * depth * hid, transcendentals=2 * rows * hid, bytes_accessed=12 * depth * hid
        ),
        compiler_params=pltpu.CompilerParams(vmem_limit_bytes=(26 << 20) + rows * (32 << 10)),
        name="expert_rows",
    )(*pieces, *own, *other)


def layer(
    queries,
    keys,
    values,
    resid_in,
    span_order,
    out_weight,
    norm_gain,
    router,
    expert_ids,
    w_gate,
    w_up,
    w_down,
):
    me = lax.axis_index("ctx")
    mine = lax.axis_index("exp").astype(i32)
    my_z, my_x, my_core = me // 8, (me // 2) % RING, me % 2

    kv = jnp.concatenate((keys, values), axis=1)
    near = join(kv, shift(kv, 1, 1), shift(kv, 1, -1), shift(kv, 1, 2))
    left, right = shift(near, 2, 1), shift(near, 2, -1)
    far = shift(near, 2, 2)

    def block_positions(seconds):
        spans = []
        for second in seconds:
            for core in (my_core, 1 - my_core):
                a = jnp.array([0, -1, 1, 2], i32)
                z = jnp.where(core == 0, my_z + second, my_z + a) % RING
                x = jnp.where(core == 0, my_x + a, my_x + second) % RING
                block = z * 8 + x * 2 + core
                spans.append((block[:, None] * 2 + jnp.arange(2, dtype=i32)[None, :]).reshape(-1))
        return positions_of(jnp.concatenate(spans), span_order).reshape(2 * len(seconds), -1)

    query_pos = positions_of(me * 2 + jnp.arange(2, dtype=i32), span_order)
    query_pos = jnp.broadcast_to(query_pos[:, None], (query_pos.shape[0], HEAD_SIZE))
    near_other, far_other = swap(near), swap(far)
    left_other, right_other = swap(left), swap(right)
    sum0, sum1, sum2, sum3 = attend(
        mine.reshape(1),
        queries,
        query_pos,
        block_positions((0, -1, 1, 2)),
        (near, near_other, left, left_other, right, right_other, far, far_other),
        out_weight,
    )

    sub = resid_in.shape[0]
    back2, back1, back3 = shift_exp(sum2, 2), shift_exp(sum1, 1), shift_exp(sum3, 3)
    own_sum = (sum0 + back2.astype(f32)) + (back1.astype(f32) + back3.astype(f32))
    stream = (resid_in.astype(f32) + own_sum).astype(bf16)
    stream_wide = stream.astype(f32)
    mean_square = jnp.mean(stream_wide * stream_wide, axis=-1, keepdims=True)
    normed = (stream_wide * lax.rsqrt(mean_square + 1e-05) * norm_gain).astype(bf16)
    logits = jnp.dot(normed.astype(f32), router, precision=lax.Precision.HIGHEST)
    experts = router.shape[1]
    expert_axis = (mine + jnp.arange(experts, dtype=i32)) % experts
    picked = expert_ids[:, :, None] == jnp.arange(experts, dtype=i32)[None, None, :]
    chosen = jnp.sum(jnp.where(picked, logits[:, None, :], 0.0), axis=-1)
    mixing = jax.nn.softmax(chosen, axis=-1)
    picked = expert_ids[:, :, None] == expert_axis[None, None, :]
    token_weight = jnp.sum(jnp.where(picked, mixing[:, :, None], 0.0), axis=1)
    routed = jnp.any(picked, axis=1)
    rank_of = jnp.cumsum(routed.astype(i32), axis=0) - 1
    slot_count = sub * expert_ids.shape[1] // experts
    slot_axis = jnp.arange(slot_count, dtype=i32)
    placing = jnp.logical_and(routed.T[:, None, :], rank_of.T[:, None, :] == slot_axis[None, :, None])
    outgoing = jnp.dot(
        placing.reshape(experts * slot_count, sub).astype(bf16), normed, preferred_element_type=f32
    ).astype(bf16)
    o0, o1, o2, o3 = (outgoing[i * slot_count : (i + 1) * slot_count] for i in range(4))
    rows = join(o0, shift_exp(o1, 1), shift_exp(o2, 2), shift_exp(o3, 3))

    own = (w_gate[0].T, w_up[0].T, w_down[0])
    other = tuple(swap(w) for w in own)
    half = rows.shape[0] // 2
    beside0, beside1 = shift(rows, 1, 1), shift(rows, 1, -1)
    n0 = join(rows, beside0)
    n1 = join(beside1, shift(beside0[:half], 1, 1), shift(beside1[half:], 1, -1))
    l0, r0 = shift(n0, 2, 1), shift(n0, 2, -1)
    r1, l1 = shift(n1, 2, -1), shift(n1, 2, 1)
    f0, f1 = shift(l0, 2, 1), shift(r1, 2, -1)

    n0, n1 = expert_rows((n0, n1), own, other)
    l0, r1 = expert_rows((l0, r1), own, other)
    l1, r0 = expert_rows((l1, r0), own, other)
    f0, f1 = expert_rows((f0, f1), own, other)

    u1, v0 = shift(l1, 2, -1), shift(r0, 2, 1)
    q0, q1 = shift(f0, 2, -1), shift(f1, 2, 1)
    u0, v1 = shift(total(l0, q0), 2, -1), shift(total(r1, q1), 2, 1)
    level = lax.ppermute(v1[:16, :128], "ctx", [(2 * i, 2 * i + 1) for i in range(16)])
    n0, n1 = total(n0, u0, v0), total(n1, u1, v1)
    part = rows.shape[0]
    half = part // 2
    minus, plus = n0[part:], n1[:part]
    q0 = shift(n1[part : part + half], 1, -1)
    q1 = shift(n1[part + half :], 1, 1)
    minus = total(minus, jnp.pad(q0, ((0, half), (0, 0))))
    plus = total(plus, jnp.pad(q1, ((half, 0), (0, 0))))
    back = (shift(minus, 1, -1), shift(plus, 1, 1))
    own_rows = total(n0[:part] + jnp.max(level) * 0, *back)

    r0, r1, r2, r3 = (own_rows[i * slot_count : (i + 1) * slot_count] for i in range(4))
    returned = join(r0, shift_exp(r1, 3), shift_exp(r2, 2), shift_exp(r3, 1))
    coefficient = placing.astype(f32) * token_weight.T[:, None, :]
    combined = jnp.einsum("est,esd->td", coefficient, returned.reshape(experts, slot_count, -1).astype(f32))
    return (stream_wide + combined).astype(bf16)


def solution(mesh):
    placed = (
        P("ctx", "exp"),
        P("ctx", "exp"),
        P("ctx", "exp"),
        P(("ctx", "exp"), None),
        P(),
        P("exp", None),
        P(),
        P(),
        P(("ctx", "exp"), None),
        P("exp", None, "ctx"),
        P("exp", None, "ctx"),
        P("exp", "ctx", None),
    )
    return jax.shard_map(layer, mesh=mesh, in_specs=placed, out_specs=P(("ctx", "exp"), None), check_vma=False)
```

```python
import math

import jax
import jax.numpy as jnp
from jax import lax
from jax.experimental import pallas as pl
from jax.experimental.pallas import tpu as pltpu
from jax.sharding import PartitionSpec as P

HEAD_SIZE = 128
SPAN = 64
RING = 4
NEVER = -1e30

f32 = jnp.float32
bf16 = jnp.bfloat16
i32 = jnp.int32


def ctx_index_of(z, x, core):
    return (z % RING) * 8 + (x % RING) * 2 + core


def ring_pairs(phase, step):
    pairs = []
    for z in range(RING):
        for x in range(RING):
            for core in range(2):
                along_x = (core == 0) == (phase == 1)
                target = ctx_index_of(z, x + step, core) if along_x else ctx_index_of(z + step, x, core)
                pairs.append((ctx_index_of(z, x, core), target))
    return pairs


RINGS = {(phase, step): ring_pairs(phase, step) for phase in (1, 2) for step in (1, -1, 2)}
SWAP = [(i, i ^ 1) for i in range(32)]


def shift(a, phase, step):
    return lax.ppermute(a, "ctx", RINGS[phase, step])


def swap(a):
    return lax.ppermute(a, "ctx", SWAP)


def shift_exp(a, step):
    return lax.ppermute(a, "exp", [(i, (i + step) % 4) for i in range(4)])


def join(*parts):
    return jnp.concatenate(parts, axis=0)


def total(*terms):
    return sum(t.astype(f32) for t in terms).astype(bf16)


def positions_of(span_ids, span_order):
    matches = span_ids[:, None] == jnp.arange(span_order.shape[0], dtype=i32)[None, :]
    starts = jnp.sum(jnp.where(matches, span_order[None, :], 0), axis=1) * SPAN
    return (starts[:, None] + jnp.arange(SPAN, dtype=i32)[None, :]).reshape(-1)


def vmem_spec():
    return pl.BlockSpec(memory_space=pltpu.VMEM)


def attend(mine, q, qpos, kpos, kvs, out_weight):
    tok = q.shape[0]
    heads = q.shape[1] // HEAD_SIZE
    kv_heads = kvs[0].shape[1] // (2 * HEAD_SIZE)
    cluster = heads // kv_heads
    rows = cluster * tok
    sub = tok // 4
    width = out_weight.shape[1]
    count = len(kvs)
    slope = math.log2(math.e) / math.sqrt(HEAD_SIZE)

    def kernel(mine_ref, q_ref, qpos_ref, kpos_ref, *refs):
        kv_refs, weight_hbm = refs[:count], refs[count]
        outs = refs[count + 1 : count + 5]
        attended, ordered, weight, sem = refs[count + 5 :]
        fetch = pltpu.make_async_copy(weight_hbm, weight, sem)
        fetch.start()

        @pl.loop(0, kv_heads)
        def _(h):
            def column(i):
                return pl.ds(pl.multiple_of(i * HEAD_SIZE, HEAD_SIZE), HEAD_SIZE)

            q_rows = jnp.concatenate([q_ref[:, column(h * cluster + g)] for g in range(cluster)], axis=0)

            def score(kv):
                contract = (((1,), (1,)), ((), ()))
                return lax.dot_general(q_rows, kv[:, column(h)], contract, preferred_element_type=f32)

            ahead = score(kv_refs[0])
            for n, kv in enumerate(kv_refs):
                s = ahead
                if n + 1 < count:
                    ahead = score(kv_refs[n + 1])
                v = kv[:, column(kv_heads + h)]
                mask = jnp.where(kpos_ref[n : n + 1, :] <= qpos_ref[:, 0:1], 0.0, NEVER)
                s = (s.reshape(cluster, tok, -1) * slope + mask[None]).reshape(rows, -1)
                top = jnp.max(s, axis=1, keepdims=True)
                if n == 0:
                    m = top
                    p = jnp.exp2(s - m)
                    l = jnp.sum(p, axis=1, keepdims=True)
                    acc = jnp.dot(p.astype(bf16), v, preferred_element_type=f32)
                else:
                    new = jnp.maximum(m, top)
                    fade = jnp.exp2(m - new)
                    p = jnp.exp2(s - new)
                    l = l * fade + jnp.sum(p, axis=1, keepdims=True)
                    acc = acc * fade + jnp.dot(p.astype(bf16), v, preferred_element_type=f32)
                    m = new
            result = (acc / l).astype(bf16)
            for g in range(cluster):
                attended[:, column(h * cluster + g)] = result[g * tok : (g + 1) * tok]

        for r in range(4):
            start = pl.multiple_of(lax.rem(mine_ref[0] + r, 4) * sub, sub)
            ordered[r * sub : (r + 1) * sub, :] = attended[pl.ds(start, sub), :]
        fetch.wait()

        @pl.loop(0, 4)
        def _(n):
            at = pl.ds(pl.multiple_of(n * (width // 4), width // 4), width // 4)
            product = jnp.dot(ordered[...], weight[:, at], preferred_element_type=f32)
            for r in range(4):
                outs[r][:, at] = product[r * sub : (r + 1) * sub].astype(outs[r].dtype)

    work = q.shape[0] * q.shape[1] * sum(kv.shape[0] for kv in kvs)
    return pl.pallas_call(
        kernel,
        out_shape=tuple(jax.ShapeDtypeStruct((sub, width), t) for t in (f32, bf16, bf16, bf16)),
        in_specs=[pl.BlockSpec(memory_space=pltpu.SMEM)] + [vmem_spec()] * (count + 3)
        + [pl.BlockSpec(memory_space=pltpu.HBM)],
        out_specs=(vmem_spec(),) * 4,
        scratch_shapes=[
            pltpu.VMEM((tok, q.shape[1]), bf16),
            pltpu.VMEM((tok, q.shape[1]), bf16),
            pltpu.VMEM(out_weight.shape, bf16),
            pltpu.SemaphoreType.DMA,
        ],
        cost_estimate=pl.CostEstimate(
            flops=8 * work, transcendentals=work // HEAD_SIZE, bytes_accessed=4 << 20
        ),
        compiler_params=pltpu.CompilerParams(vmem_limit_bytes=52 << 20),
        name="attend",
    )(mine, q, qpos, kpos, *kvs, out_weight)


def expert_rows(pieces, own, other):
    hid, depth = own[0].shape
    width = own[2].shape[1]
    chunks, panels = 4, 4
    deep, wide = depth // chunks, width // panels
    sizes = [p.shape[0] for p in pieces]
    rows = sum(sizes)
    count = len(pieces)
    starts = [sum(sizes[:i]) for i in range(count)]

    def kernel(*refs):
        ins, refs = refs[:count], refs[count:]
        (ga, ua, da, gb, ub, db), refs = refs[:6], refs[6:]
        outs, refs = refs[:count], refs[count:]
        x, w, dw, sums, hidden, out, x_sems, w_sems, d_sems, out_sems = refs

        def first_copies(k):
            at = pl.ds(pl.multiple_of(k * deep, deep), deep)
            for i, ref in enumerate((ga, gb, ua, ub)):
                yield pltpu.make_async_copy(ref.at[:, at], w.at[k, pl.ds(i * hid, hid), :], w_sems.at[k, i])
            for i, ref in enumerate(ins):
                yield pltpu.make_async_copy(
                    ref.at[:, at], x.at[k, pl.ds(starts[i], sizes[i]), :], x_sems.at[k, i]
                )

        def last_copies(n):
            at = pl.ds(pl.multiple_of(n * wide, wide), wide)
            for i, ref in enumerate((da, db)):
                yield pltpu.make_async_copy(ref.at[:, at], dw.at[n, pl.ds(i * hid, hid), :], d_sems.at[n, i])

        def out_copies(n):
            at = pl.ds(pl.multiple_of(n * wide, wide), wide)
            for i, ref in enumerate(outs):
                yield pltpu.make_async_copy(
                    out.at[n, pl.ds(starts[i], sizes[i]), :], ref.at[:, at], out_sems.at[n, i]
                )

        for k in range(chunks):
            for copy in first_copies(k):
                copy.start()
        for n in range(panels):
            for copy in last_copies(n):
                copy.start()
        sums[...] = jnp.zeros_like(sums)

        @pl.loop(0, chunks)
        def _(k):
            for copy in first_copies(k):
                copy.wait()
            sums[...] += lax.dot_general(x[k], w[k], (((1,), (1,)), ((), ())), preferred_element_type=f32)

        hidden[...] = (jax.nn.silu(sums[:, : 2 * hid]) * sums[:, 2 * hid :]).astype(bf16)

        @pl.loop(0, panels)
        def _(n):
            for copy in last_copies(n):
                copy.wait()
            out[n] = jnp.dot(hidden[...], dw[n], preferred_element_type=f32).astype(bf16)
            for copy in out_copies(n):
                copy.start()

        for n in range(panels):
            for copy in out_copies(n):
                copy.wait()

    anywhere = pl.BlockSpec(memory_space=pltpu.HBM)
    return pl.pallas_call(
        kernel,
        out_shape=tuple(jax.ShapeDtypeStruct((size, width), bf16) for size in sizes),
        in_specs=[anywhere] * (count + 6),
        out_specs=(anywhere,) * count,
        scratch_shapes=[
            pltpu.VMEM((chunks, rows, deep), bf16),
            pltpu.VMEM((chunks, 4 * hid, deep), bf16),
            pltpu.VMEM((panels, 2 * hid, wide), bf16),
            pltpu.VMEM((rows, 4 * hid), f32),
            pltpu.VMEM((rows, 2 * hid), bf16),
            pltpu.VMEM((panels, rows, wide), bf16),
            pltpu.SemaphoreType.DMA((chunks, count)),
            pltpu.SemaphoreType.DMA((chunks, 4)),
            pltpu.SemaphoreType.DMA((panels, 2)),
            pltpu.SemaphoreType.DMA((panels, count)),
        ],
        cost_estimate=pl.CostEstimate(
            flops=12 * rows * depth * hid, transcendentals=2 * rows * hid, bytes_accessed=12 * depth * hid
        ),
        compiler_params=pltpu.CompilerParams(vmem_limit_bytes=(26 << 20) + rows * (32 << 10)),
        name="expert_rows",
    )(*pieces, *own, *other)


def layer(
    queries,
    keys,
    values,
    resid_in,
    span_order,
    out_weight,
    norm_gain,
    router,
    expert_ids,
    w_gate,
    w_up,
    w_down,
):
    me = lax.axis_index("ctx")
    mine = lax.axis_index("exp").astype(i32)
    my_z, my_x, my_core = me // 8, (me // 2) % RING, me % 2

    beside = ((0, 0), (0, keys.shape[1]))
    kv = jnp.pad(keys, beside) + jnp.pad(values, tuple(side[::-1] for side in beside))
    near = join(kv, shift(kv, 1, 1), shift(kv, 1, -1), shift(kv, 1, 2))
    left, right = shift(near, 2, 1), shift(near, 2, -1)
    far = shift(near, 2, 2)

    def block_positions(seconds):
        spans = []
        for second in seconds:
            for core in (my_core, 1 - my_core):
                a = jnp.array([0, -1, 1, 2], i32)
                z = jnp.where(core == 0, my_z + second, my_z + a) % RING
                x = jnp.where(core == 0, my_x + a, my_x + second) % RING
                block = z * 8 + x * 2 + core
                spans.append((block[:, None] * 2 + jnp.arange(2, dtype=i32)[None, :]).reshape(-1))
        return positions_of(jnp.concatenate(spans), span_order).reshape(2 * len(seconds), -1)

    query_pos = positions_of(me * 2 + jnp.arange(2, dtype=i32), span_order)
    query_pos = jnp.broadcast_to(query_pos[:, None], (query_pos.shape[0], HEAD_SIZE))
    near_other, far_other = swap(near), swap(far)
    left_other, right_other = swap(left), swap(right)
    sum0, sum1, sum2, sum3 = attend(
        mine.reshape(1),
        queries,
        query_pos,
        block_positions((0, -1, 1, 2)),
        (near, near_other, left, left_other, right, right_other, far, far_other),
        out_weight,
    )

    sub = resid_in.shape[0]
    back2, back1, back3 = shift_exp(sum2, 2), shift_exp(sum1, 1), shift_exp(sum3, 3)
    own_sum = (sum0 + back2.astype(f32)) + (back1.astype(f32) + back3.astype(f32))
    stream = (resid_in.astype(f32) + own_sum).astype(bf16)
    stream_wide = stream.astype(f32)
    mean_square = jnp.mean(stream_wide * stream_wide, axis=-1, keepdims=True)
    normed = (stream_wide * lax.rsqrt(mean_square + 1e-05) * norm_gain).astype(bf16)
    logits = jnp.dot(normed.astype(f32), router, precision=lax.Precision.HIGHEST)
    experts = router.shape[1]
    expert_axis = (mine + jnp.arange(experts, dtype=i32)) % experts
    picked = expert_ids[:, :, None] == jnp.arange(experts, dtype=i32)[None, None, :]
    chosen = jnp.sum(jnp.where(picked, logits[:, None, :], 0.0), axis=-1)
    mixing = jax.nn.softmax(chosen, axis=-1)
    picked = expert_ids[:, :, None] == expert_axis[None, None, :]
    token_weight = jnp.sum(jnp.where(picked, mixing[:, :, None], 0.0), axis=1)
    routed = jnp.any(picked, axis=1)
    rank_of = jnp.cumsum(routed.astype(i32), axis=0) - 1
    slot_count = sub * expert_ids.shape[1] // experts
    slot_axis = jnp.arange(slot_count, dtype=i32)
    placing = jnp.logical_and(routed.T[:, None, :], rank_of.T[:, None, :] == slot_axis[None, :, None])
    outgoing = jnp.dot(
        placing.reshape(experts * slot_count, sub).astype(bf16), normed, preferred_element_type=f32
    ).astype(bf16)
    o0, o1, o2, o3 = (outgoing[i * slot_count : (i + 1) * slot_count] for i in range(4))
    rows = join(o0, shift_exp(o1, 1), shift_exp(o2, 2), shift_exp(o3, 3))

    own = (w_gate[0].T, w_up[0].T, w_down[0])
    other = tuple(swap(w) for w in own)
    half = rows.shape[0] // 2
    beside0, beside1 = shift(rows, 1, 1), shift(rows, 1, -1)
    n0 = join(rows, beside0)
    n1 = join(beside1, shift(beside0[:half], 1, 1), shift(beside1[half:], 1, -1))
    l0, r0 = shift(n0, 2, 1), shift(n0, 2, -1)
    r1, l1 = shift(n1, 2, -1), shift(n1, 2, 1)
    f0, f1 = shift(l0, 2, 1), shift(r1, 2, -1)

    n0, n1 = expert_rows((n0, n1), own, other)
    l0, r1 = expert_rows((l0, r1), own, other)
    l1, r0 = expert_rows((l1, r0), own, other)
    f0, f1 = expert_rows((f0, f1), own, other)

    u1, v0 = shift(l1, 2, -1), shift(r0, 2, 1)
    q0, q1 = shift(f0, 2, -1), shift(f1, 2, 1)
    u0, v1 = shift(total(l0, q0), 2, -1), shift(total(r1, q1), 2, 1)
    level = lax.ppermute(v1[:16, :128], "ctx", [(2 * i, 2 * i + 1) for i in range(16)])
    n0, n1 = total(n0, u0, v0), total(n1, u1, v1)
    part = rows.shape[0]
    back = (shift(n0[part:], 1, -1), shift(n1[:part], 1, 1), shift(n1[part:], 1, 2))
    own_rows = total(n0[:part] + jnp.max(level) * 0, *back)

    r0, r1, r2, r3 = (own_rows[i * slot_count : (i + 1) * slot_count] for i in range(4))
    returned = join(r0, shift_exp(r1, 3), shift_exp(r2, 2), shift_exp(r3, 1))
    coefficient = placing.astype(f32) * token_weight.T[:, None, :]
    combined = jnp.einsum("est,esd->td", coefficient, returned.reshape(experts, slot_count, -1).astype(f32))
    return (stream_wide + combined).astype(bf16)


def solution(mesh):
    placed = (
        P("ctx", "exp"),
        P("ctx", "exp"),
        P("ctx", "exp"),
        P(("ctx", "exp"), None),
        P(),
        P("exp", None),
        P(),
        P(),
        P(("ctx", "exp"), None),
        P("exp", None, "ctx"),
        P("exp", None, "ctx"),
        P("exp", "ctx", None),
    )
    return jax.shard_map(layer, mesh=mesh, in_specs=placed, out_specs=P(("ctx", "exp"), None), check_vma=False)
```
